128 devices in a mesh: rows: 64 (over z, y, x), cols: 2 (over core).
Axes of the slice: x: 4, y: 4, z: 4, core: 2. Of those that a mesh axis runs over, the one named last changes fastest.
Arguments:
- embeddings: bfloat16 [196608, 1536], P('rows'), may hold values from -43 to 43, as said below
- start_basis: float32 [1536, 256], P(None, 'cols'), may hold values from -6 to 6
Outputs:
- projected: bfloat16 [196608, 256], P('rows', 'cols')
- basis: float32 [1536, 256], P(None, 'cols')
The draws below stay inside these ranges and needn't reach their ends.
Inputs may be any that keep to these rules, and one draw needn't show every extreme that they name: `embeddings`: rows are noisy vectors around offsets that differ between aligned blocks of rows, with per-column spreads that differ by a factor of up to four.
All inputs are finite; a program needn't handle non-finite values.
Results may differ from the reference program's by a relative error of at most 0.025.
Values may be sent and summed in bfloat16 or wider, within the bound.
A program may use at most 64 MiB of HBM per device.

```python
import jax
import jax.numpy as jnp
from jax import lax

D = 1536
K = 256
ROW_DEV = 3072
ITERS = 3
ROWS = 196608


def draw_embeddings(key, part):
    key_offset, key_scale, key_noise = jax.random.split(key, 3)
    key_blocks = jax.random.fold_in(key, 7919)
    offset = jnp.clip(jax.random.normal(key_offset, (D,), jnp.float32), -3.0, 3.0)
    col_scale = jnp.exp(jax.random.uniform(key_scale, (D,), jnp.float32, -0.69, 0.69))
    block_shift = jnp.clip(0.8 * jax.random.normal(key_blocks, (ROWS // ROW_DEV, D), jnp.float32), -3.0, 3.0)
    row_shift = jnp.repeat(block_shift, ROW_DEV, axis=0, total_repeat_length=ROWS)
    noise = jnp.clip(jax.random.normal(key_noise, (ROWS, D), jnp.float32), -5.0, 5.0)
    values = noise * col_scale[None, :] + offset[None, :] + row_shift
    return values.astype(jnp.bfloat16)


def block_scale(rng, extent, pieces, smallest, high):
    def one(dim, blocks):
        steps = jax.random.uniform(jax.random.fold_in(jax.random.fold_in(rng, 6), dim), (blocks,), jnp.float32, smallest / len(pieces), high / len(pieces))
        return jnp.repeat(jnp.exp(steps), extent[dim] // blocks).reshape((-1,) + (1,) * (len(extent) - dim - 1))

    gain = one(*pieces[0])
    for cut in pieces[1:]:
        gain = gain * one(*cut)
    return gain


def normal_values(own_key, shape, width, limit, cuts=(), held_as=jnp.bfloat16):
    values = width * jax.random.normal(own_key, shape, jnp.float32)
    if cuts:
        values = values * block_scale(own_key, shape, cuts, -0.22, 0.18)
    return jnp.clip(values, -limit, limit).astype(held_as)


def setup_inputs(seed: int = 0) -> dict:
    streams_of = jax.random.split(jax.random.key(seed), 3)
    return {
        "embeddings": draw_embeddings(jax.random.fold_in(streams_of[2], 71), 0),
        "start_basis": normal_values(streams_of[1], (D, K), 1.0, 6.0, ((1, 2),), jnp.float32),
    }


def reference(embeddings, start_basis):
    rows_count = embeddings.shape[0]
    col_mean = lax.optimization_barrier(jnp.sum(embeddings, axis=0, dtype=jnp.float32)) / rows_count
    basis = start_basis
    for sweep_index in range(ITERS):
        basis_bf = basis.astype(jnp.bfloat16)
        raw_proj = jnp.dot(embeddings.astype(jnp.float32), basis_bf.astype(jnp.float32), preferred_element_type=jnp.float32)
        offset = jnp.dot(col_mean, basis_bf.astype(jnp.float32), precision=lax.Precision.HIGHEST)
        shifted = (raw_proj - offset[None, :]).astype(jnp.bfloat16)
        col_sums = lax.optimization_barrier(jnp.sum(shifted, axis=0, dtype=jnp.float32))
        products = lax.dot_general(embeddings.astype(jnp.float32), shifted.astype(jnp.float32), (((0,), (0,)), ((), ())), preferred_element_type=jnp.float32)
        products = products - col_mean[:, None] * col_sums[None, :]
        gram_matrix = jnp.dot(products.T, products, precision=lax.Precision.HIGHEST)
        lower = jnp.linalg.cholesky(gram_matrix)
        basis = lax.linalg.triangular_solve(lower, products, left_side=False, lower=True, transpose_a=True)
    centered = embeddings.astype(jnp.float32) - col_mean[None, :]
    unit = (centered * lax.rsqrt(lax.optimization_barrier(jnp.sum(centered * centered, axis=1, keepdims=True)) + 1.0)).astype(jnp.bfloat16)
    coords = jnp.dot(unit.astype(jnp.float32), basis.astype(jnp.bfloat16).astype(jnp.float32), preferred_element_type=jnp.float32)
    scaled = coords * lax.rsqrt(lax.optimization_barrier(jnp.mean(coords * coords, axis=1, keepdims=True)) + 0.0001)
    return (scaled.astype(jnp.bfloat16), basis)
```

```python
import functools

import jax
import jax.numpy as jnp
from jax import lax
from jax.experimental import pallas as pl
from jax.experimental.pallas import tpu as pltpu
from jax.sharding import PartitionSpec as P

D = 1536
K = 256
B = 256
NB = D // B
OFFS = 4
MESH = pl.DeviceIdType.MESH
VMEM = pltpu.VMEM
F32 = jnp.float32
BF16 = jnp.bfloat16
STRIDES = (1, 4, 16)
STEP_ROWS = 512


def moment_kernel(steps, rows, e_ref, s_ref, mu_ref, acc, sums):
    step = pl.program_id(0)
    core = lax.axis_index("cols")
    total = None
    for r in range(0, e_ref.shape[0], 8):
        part = e_ref[pl.ds(r, 8), :].astype(F32)
        total = part if total is None else total + part

    @pl.when(step == 0)
    def _():
        sums[...] = total

    @pl.when(step > 0)
    def _():
        sums[...] += total

    for k in range(3):
        i = core * 3 + k
        left = e_ref[:, pl.ds(pl.multiple_of(i * B, B), B)]
        for o in range(OFFS):
            j = lax.rem(i + o, NB)
            right = e_ref[:, pl.ds(pl.multiple_of(j * B, B), B)]
            new = lax.dot_general(
                left, right, (((0,), (0,)), ((), ())), preferred_element_type=F32
            )
            at = (k * OFFS + o) * B

            @pl.when(step == 0)
            def _():
                acc[pl.ds(at, B), :] = new

            @pl.when(step > 0)
            def _():
                acc[pl.ds(at, B), :] += new

    @pl.when(step == steps - 1)
    def _():
        whole = jnp.sum(sums[...], axis=0, keepdims=True)
        keep = lax.broadcasted_iota(jnp.int32, (8, D), 0) == 0
        sums[...] = jnp.where(keep, jnp.broadcast_to(whole, (8, D)), 0.0)
        for k in range(3):
            i = core * 3 + k
            left = sums[:, pl.ds(pl.multiple_of(i * B, B), B)]
            mu_ref[2 * k : 2 * k + 1, :] = left[0:1, :128] / rows
            mu_ref[2 * k + 1 : 2 * k + 2, :] = left[0:1, 128:] / rows
            for o in range(OFFS):
                j = lax.rem(i + o, NB)
                right = sums[:, pl.ds(pl.multiple_of(j * B, B), B)]
                outer = lax.dot_general(
                    left,
                    right / rows,
                    (((0,), (0,)), ((), ())),
                    preferred_element_type=F32,
                    precision=lax.Precision.HIGHEST,
                )
                at = (k * OFFS + o) * B
                s_ref[pl.ds(at, B), :] = (acc[pl.ds(at, B), :] - outer).astype(BF16)
        mu_ref[6:8, :] = jnp.zeros((2, 128), F32)


def local_moment(embeddings):
    rows = embeddings.shape[0]
    steps = rows // STEP_ROWS
    size = 3 * OFFS * B
    return pl.pallas_call(
        functools.partial(moment_kernel, steps, rows),
        grid=(steps,),
        out_shape=(
            jax.ShapeDtypeStruct((size, B), BF16),
            jax.ShapeDtypeStruct((8, 128), F32),
        ),
        in_specs=[pl.BlockSpec((STEP_ROWS, D), lambda s: (s, 0))],
        out_specs=(
            pl.BlockSpec((size, B), lambda s: (0, 0)),
            pl.BlockSpec((8, 128), lambda s: (0, 0)),
        ),
        scratch_shapes=[VMEM((size, B), F32), VMEM((8, D), F32)],
        compiler_params=pltpu.CompilerParams(
            vmem_limit_bytes=40 * 2**20, dimension_semantics=("arbitrary",)
        ),
        name="moment",
    )(embeddings)


def exchange_kernel(
    s_ref, mu_ref, b_ref,
    c_out, mu_out, b_out,
    got1, got2, got3, part2, part3,
    send_rs, recv_rs, send_ag, recv_ag, send_cc, recv_cc, send_mu, recv_mu, send_x, recv_x,
):
    me = lax.axis_index("rows")
    core = lax.axis_index("cols")
    other = 1 - core
    coord = [lax.rem(me // s, 4) for s in STRIDES]

    def peer(dim, o):
        return me + (lax.rem(coord[dim] + o, 4) - coord[dim]) * STRIDES[dim]

    barrier = pltpu.get_barrier_semaphore()
    for dim in range(3):
        for o in (1, 2, 3):
            pl.semaphore_signal(barrier, inc=1, device_id=(peer(dim, o), core), device_id_type=MESH)
    pl.semaphore_signal(barrier, inc=1, device_id=(me, other), device_id_type=MESH)
    pl.semaphore_wait(barrier, 10)

    started = []

    def send(src, dst, send_sem, recv_sem, to):
        copy = pltpu.make_async_remote_copy(
            src_ref=src, dst_ref=dst, send_sem=send_sem, recv_sem=recv_sem,
            device_id=to, device_id_type=MESH,
        )
        copy.start()
        started.append(copy)
        return copy

    def rows_of(k, start, size):
        return pl.ds(pl.multiple_of(k * 1024 + start, 16), size)

    first = {}
    for o in (1, 3, 2):
        for k in range(3):
            to = lax.rem(coord[k] + o, 4)
            first[k, o] = send(
                s_ref.at[rows_of(k, to * 256, 256)], got1.at[k, o - 1],
                send_rs.at[0, k, o - 1], recv_rs.at[0, k, o - 1], (peer(k, o), core),
            )
    mu_out[core, me] = mu_ref[...]
    mu1 = [
        send(
            mu_ref, mu_out.at[core, me], send_mu.at[0, o - 1], recv_mu.at[0, o - 1],
            (peer(0, o), core),
        )
        for o in (1, 2, 3)
    ]
    b_copy = send(b_ref, b_out.at[core], send_x.at[0], recv_x.at[0], (me, other))
    b_out[core] = b_ref[...]

    second = {}
    for k in range(3):
        for o in (1, 2, 3):
            first[k, o].wait_recv()
        total = s_ref[rows_of(k, coord[k] * 256, 256), :].astype(F32)
        for o in range(3):
            total = total + got1[k, o].astype(F32)
        part2[k] = total.astype(BF16)
        d = (k + 1) % 3
        for o in (1, 3, 2):
            to = lax.rem(coord[d] + o, 4)
            second[k, o] = send(
                part2.at[k, pl.ds(pl.multiple_of(to * 64, 16), 64)], got2.at[k, o - 1],
                send_rs.at[1, k, o - 1], recv_rs.at[1, k, o - 1], (peer(d, o), core),
            )
    for copy in mu1:
        copy.wait_recv()
    line = pl.multiple_of(me // 4 * 4, 4)
    mu2 = [
        send(
            mu_out.at[core, pl.ds(line, 4)], mu_out.at[core, pl.ds(line, 4)],
            send_mu.at[1, o - 1], recv_mu.at[1, o - 1], (peer(1, o), core),
        )
        for o in (1, 2, 3)
    ]
    third = {}
    for k in range(3):
        d = (k + 1) % 3
        for o in (1, 2, 3):
            second[k, o].wait_recv()
        total = part2[k, pl.ds(pl.multiple_of(coord[d] * 64, 16), 64), :].astype(F32)
        for o in range(3):
            total = total + got2[k, o].astype(F32)
        part3[k] = total.astype(BF16)
        d = (k + 2) % 3
        for o in (1, 3, 2):
            to = lax.rem(coord[d] + o, 4)
            third[k, o] = send(
                part3.at[k, pl.ds(pl.multiple_of(to * 16, 16), 16)], got3.at[k, o - 1],
                send_rs.at[2, k, o - 1], recv_rs.at[2, k, o - 1], (peer(d, o), core),
            )
    for copy in mu2:
        copy.wait_recv()
    plane = pl.multiple_of(me // 16 * 16, 16)
    mu3 = [
        send(
            mu_out.at[core, pl.ds(plane, 16)], mu_out.at[core, pl.ds(plane, 16)],
            send_mu.at[2, o - 1], recv_mu.at[2, o - 1], (peer(2, o), core),
        )
        for o in (1, 2, 3)
    ]
    spread = {}
    for k in range(3):
        a, b, c = (coord[(k + n) % 3] for n in range(3))
        d = (k + 2) % 3
        for o in (1, 2, 3):
            third[k, o].wait_recv()
        total = part3[k, pl.ds(pl.multiple_of(c * 16, 16), 16), :].astype(F32)
        for o in range(3):
            total = total + got3[k, o].astype(F32)
        mine = rows_of(k, (a * 16 + b * 4 + c) * 16, 16)
        c_out[core, mine, :] = total.astype(BF16)
        for o in (1, 3, 2):
            spread[0, k, o] = send(
                c_out.at[core, mine], c_out.at[core, mine],
                send_ag.at[0, k, o - 1], recv_ag.at[0, k, o - 1], (peer(d, o), core),
            )
    for k in range(3):
        a, b = (coord[(k + n) % 3] for n in range(2))
        d = (k + 1) % 3
        for o in (1, 2, 3):
            spread[0, k, o].wait_recv()
        mine = rows_of(k, (a * 4 + b) * 64, 64)
        for o in (1, 3, 2):
            spread[1, k, o] = send(
                c_out.at[core, mine], c_out.at[core, mine],
                send_ag.at[1, k, o - 1], recv_ag.at[1, k, o - 1], (peer(d, o), core),
            )
    across = []
    for k in range(3):
        a = coord[k]
        for o in (1, 2, 3):
            spread[1, k, o].wait_recv()
        mine = rows_of(k, a * 256, 256)
        for o in (1, 3, 2):
            spread[2, k, o] = send(
                c_out.at[core, mine], c_out.at[core, mine],
                send_ag.at[2, k, o - 1], recv_ag.at[2, k, o - 1], (peer(k, o), core),
            )
        across.append(
            send(
                c_out.at[core, mine], c_out.at[core, mine],
                send_cc.at[k, 0], recv_cc.at[k, 0], (me, other),
            )
        )
    for copy in mu3:
        copy.wait_recv()
    mu_copy = send(mu_out.at[core], mu_out.at[core], send_x.at[1], recv_x.at[1], (me, other))
    for o in (1, 3, 2):
        for k in range(3):
            spread[2, k, o].wait_recv()
            got = rows_of(k, lax.rem(coord[k] + 4 - o, 4) * 256, 256)
            across.append(
                send(
                    c_out.at[core, got], c_out.at[core, got],
                    send_cc.at[k, o], recv_cc.at[k, o], (me, other),
                )
            )
    for copy in across:
        copy.wait_recv()
    mu_copy.wait_recv()
    b_copy.wait_recv()
    for copy in started:
        copy.wait_send()


def exchanged(s, mu, b):
    sem = pltpu.SemaphoreType.DMA
    vm = pl.BlockSpec(memory_space=VMEM)
    return pl.pallas_call(
        exchange_kernel,
        out_shape=(
            jax.ShapeDtypeStruct((2, *s.shape), BF16),
            jax.ShapeDtypeStruct((2, 64, 8, 128), F32),
            jax.ShapeDtypeStruct((2, *b.shape), BF16),
        ),
        in_specs=[vm] * 3,
        out_specs=(vm,) * 3,
        scratch_shapes=[
            VMEM((3, 3, 256, B), BF16),
            VMEM((3, 3, 64, B), BF16),
            VMEM((3, 3, 16, B), BF16),
            VMEM((3, 256, B), BF16),
            VMEM((3, 64, B), BF16),
            sem((3, 3, 3)), sem((3, 3, 3)),
            sem((3, 3, 3)), sem((3, 3, 3)),
            sem((3, 4)), sem((3, 4)),
            sem((3, 3)), sem((3, 3)),
            sem((2,)), sem((2,)),
        ],
        compiler_params=pltpu.CompilerParams(
            collective_id=0, has_side_effects=True, vmem_limit_bytes=24 * 2**20
        ),
        name="exchange",
    )(s, mu, b)


def shards(embeddings, start_basis):
    rows = embeddings.shape[0]
    core = lax.axis_index("cols")
    s, mu = local_moment(embeddings)
    c_all, mu_all, b_all = exchanged(s, mu, start_basis.T.astype(BF16))
    means = mu_all[:, :, :6, :].transpose(1, 0, 2, 3).reshape(64, D)
    mean = jnp.mean(means, axis=0)
    apart = means - mean[None, :]
    blocks = c_all.reshape(NB, OFFS, B, B)
    lines = []
    for i in range(NB):
        at = {(i + o) % NB: blocks[i, o] for o in range(OFFS)}
        for o in (4, 5):
            at[(i + o) % NB] = blocks[(i + o) % NB, NB - o].T
        lines.append(jnp.concatenate([at[j] for j in range(NB)], axis=1))
    moment = jnp.concatenate(lines, axis=0)
    high = lax.Precision.HIGHEST

    def apply(x):
        side = jnp.dot(x, apart.T, precision=high)
        whole = jnp.dot(x.astype(BF16), moment, preferred_element_type=F32)
        whole = whole + rows * jnp.dot(side, apart, precision=high)
        return whole / (rows * lax.axis_size("rows"))

    x = apply(apply(b_all.reshape(K, D).astype(F32)).astype(BF16).astype(F32))
    for last in (False, True):
        gram = jnp.dot(x, x.T, precision=high)
        lower = jnp.linalg.cholesky(gram)
        x = lax.linalg.triangular_solve(lower, x, left_side=True, lower=True)
        if not last:
            x = apply(x.astype(BF16).astype(F32))
    basis = lax.dynamic_slice_in_dim(x, core * 128, 128, 0).T
    centered = embeddings.astype(F32) - mean[None, :]
    unit = centered * lax.rsqrt(jnp.sum(centered * centered, axis=1, keepdims=True) + 1.0)
    coords = lax.dot_general(
        unit.astype(BF16), x.astype(BF16), (((1,), (1,)), ((), ())), preferred_element_type=F32
    )
    squares = jnp.sum(coords * coords, axis=1, keepdims=True)
    own = lax.dynamic_slice_in_dim(coords, core * 128, 128, 1)
    return ((own * lax.rsqrt(squares / K + 0.0001)).astype(BF16), basis)


def solution(mesh):
    in_specs = (P("rows", None), P(None, "cols"))
    out_specs = (P("rows", "cols"), P(None, "cols"))
    return jax.shard_map(shards, mesh=mesh, in_specs=in_specs, out_specs=out_specs, check_vma=False)
```

```python
import functools

import jax
import jax.numpy as jnp
from jax import lax
from jax.experimental import pallas as pl
from jax.experimental.pallas import tpu as pltpu
from jax.sharding import PartitionSpec as P

D = 1536
K = 256
B = 256
NB = D // B
OFFS = 4
MESH = pl.DeviceIdType.MESH
VMEM = pltpu.VMEM
F32 = jnp.float32
BF16 = jnp.bfloat16
STRIDES = (1, 4, 16)
STEP_ROWS = 512


def moment_kernel(steps, rows, e_ref, s_ref, mu_ref, acc, sums):
    step = pl.program_id(0)
    core = lax.axis_index("cols")
    total = None
    for r in range(0, e_ref.shape[0], 8):
        part = e_ref[pl.ds(r, 8), :].astype(F32)
        total = part if total is None else total + part

    @pl.when(step == 0)
    def _():
        sums[...] = total

    @pl.when(step > 0)
    def _():
        sums[...] += total

    for k in range(3):
        i = core * 3 + k
        left = e_ref[:, pl.ds(pl.multiple_of(i * B, B), B)]
        for o in range(OFFS):
            j = lax.rem(i + o, NB)
            right = e_ref[:, pl.ds(pl.multiple_of(j * B, B), B)]
            new = lax.dot_general(
                left, right, (((0,), (0,)), ((), ())), preferred_element_type=F32
            )
            at = (k * OFFS + o) * B

            @pl.when(step == 0)
            def _():
                acc[pl.ds(at, B), :] = new

            @pl.when(step > 0)
            def _():
                acc[pl.ds(at, B), :] += new

    @pl.when(step == steps - 1)
    def _():
        whole = jnp.sum(sums[...], axis=0, keepdims=True)
        keep = lax.broadcasted_iota(jnp.int32, (8, D), 0) == 0
        sums[...] = jnp.where(keep, jnp.broadcast_to(whole, (8, D)), 0.0)
        for k in range(3):
            i = core * 3 + k
            left = sums[:, pl.ds(pl.multiple_of(i * B, B), B)]
            mu_ref[2 * k : 2 * k + 1, :] = left[0:1, :128] / rows
            mu_ref[2 * k + 1 : 2 * k + 2, :] = left[0:1, 128:] / rows
            for o in range(OFFS):
                j = lax.rem(i + o, NB)
                right = sums[:, pl.ds(pl.multiple_of(j * B, B), B)]
                outer = lax.dot_general(
                    left,
                    right / rows,
                    (((0,), (0,)), ((), ())),
                    preferred_element_type=F32,
                    precision=lax.Precision.HIGHEST,
                )
                at = (k * OFFS + o) * B
                s_ref[pl.ds(at, B), :] = (acc[pl.ds(at, B), :] - outer).astype(BF16)
        mu_ref[6:8, :] = jnp.zeros((2, 128), F32)


def local_moment(embeddings):
    rows = embeddings.shape[0]
    steps = rows // STEP_ROWS
    size = 3 * OFFS * B
    return pl.pallas_call(
        functools.partial(moment_kernel, steps, rows),
        grid=(steps,),
        out_shape=(
            jax.ShapeDtypeStruct((size, B), BF16),
            jax.ShapeDtypeStruct((8, 128), F32),
        ),
        in_specs=[pl.BlockSpec((STEP_ROWS, D), lambda s: (s, 0))],
        out_specs=(
            pl.BlockSpec((size, B), lambda s: (0, 0)),
            pl.BlockSpec((8, 128), lambda s: (0, 0)),
        ),
        scratch_shapes=[VMEM((size, B), F32), VMEM((8, D), F32)],
        compiler_params=pltpu.CompilerParams(
            vmem_limit_bytes=40 * 2**20, dimension_semantics=("arbitrary",)
        ),
        name="moment",
    )(embeddings)


def exchange_kernel(
    s_ref, mu_ref, b_ref,
    c_out, mu_out, b_out,
    got1, got2, got3, part2, part3,
    send_rs, recv_rs, send_ag, recv_ag, send_cc, recv_cc, send_mu, recv_mu, send_x, recv_x,
):
    me = lax.axis_index("rows")
    core = lax.axis_index("cols")
    other = 1 - core
    coord = [lax.rem(me // s, 4) for s in STRIDES]

    def peer(dim, o):
        return me + (lax.rem(coord[dim] + o, 4) - coord[dim]) * STRIDES[dim]

    barrier = pltpu.get_barrier_semaphore()
    for dim in range(3):
        for o in (1, 2, 3):
            pl.semaphore_signal(barrier, inc=1, device_id=(peer(dim, o), core), device_id_type=MESH)
    pl.semaphore_signal(barrier, inc=1, device_id=(me, other), device_id_type=MESH)
    pl.semaphore_wait(barrier, 10)

    started = []

    def send(src, dst, send_sem, recv_sem, to):
        copy = pltpu.make_async_remote_copy(
            src_ref=src, dst_ref=dst, send_sem=send_sem, recv_sem=recv_sem,
            device_id=to, device_id_type=MESH,
        )
        copy.start()
        started.append(copy)
        return copy

    def rows_of(k, start, size):
        return pl.ds(pl.multiple_of(k * 1024 + start, 16), size)

    first = {}
    for o in (1, 3, 2):
        for k in range(3):
            to = lax.rem(coord[k] + o, 4)
            first[k, o] = send(
                s_ref.at[rows_of(k, to * 256, 256)], got1.at[k, o - 1],
                send_rs.at[0, k, o - 1], recv_rs.at[0, k, o - 1], (peer(k, o), core),
            )
    mu_out[core, me] = mu_ref[...]
    mu1 = [
        send(
            mu_ref, mu_out.at[core, me], send_mu.at[0, o - 1], recv_mu.at[0, o - 1],
            (peer(0, o), core),
        )
        for o in (1, 2, 3)
    ]
    b_copy = send(b_ref, b_out.at[core], send_x.at[0], recv_x.at[0], (me, other))
    b_out[core] = b_ref[...]

    second = {}
    for k in range(3):
        for o in (1, 2, 3):
            first[k, o].wait_recv()
        total = s_ref[rows_of(k, coord[k] * 256, 256), :].astype(F32)
        for o in range(3):
            total = total + got1[k, o].astype(F32)
        part2[k] = total.astype(BF16)
        d = (k + 1) % 3
        for o in (1, 3, 2):
            to = lax.rem(coord[d] + o, 4)
            second[k, o] = send(
                part2.at[k, pl.ds(pl.multiple_of(to * 64, 16), 64)], got2.at[k, o - 1],
                send_rs.at[1, k, o - 1], recv_rs.at[1, k, o - 1], (peer(d, o), core),
            )
    for copy in mu1:
        copy.wait_recv()
    line = pl.multiple_of(me // 4 * 4, 4)
    mu2 = [
        send(
            mu_out.at[core, pl.ds(line, 4)], mu_out.at[core, pl.ds(line, 4)],
            send_mu.at[1, o - 1], recv_mu.at[1, o - 1], (peer(1, o), core),
        )
        for o in (1, 2, 3)
    ]
    third = {}
    for k in range(3):
        d = (k + 1) % 3
        for o in (1, 2, 3):
            second[k, o].wait_recv()
        total = part2[k, pl.ds(pl.multiple_of(coord[d] * 64, 16), 64), :].astype(F32)
        for o in range(3):
            total = total + got2[k, o].astype(F32)
        part3[k] = total.astype(BF16)
        d = (k + 2) % 3
        for o in (1, 3, 2):
            to = lax.rem(coord[d] + o, 4)
            third[k, o] = send(
                part3.at[k, pl.ds(pl.multiple_of(to * 16, 16), 16)], got3.at[k, o - 1],
                send_rs.at[2, k, o - 1], recv_rs.at[2, k, o - 1], (peer(d, o), core),
            )
    for copy in mu2:
        copy.wait_recv()
    plane = pl.multiple_of(me // 16 * 16, 16)
    mu3 = [
        send(
            mu_out.at[core, pl.ds(plane, 16)], mu_out.at[core, pl.ds(plane, 16)],
            send_mu.at[2, o - 1], recv_mu.at[2, o - 1], (peer(2, o), core),
        )
        for o in (1, 2, 3)
    ]
    spread = {}
    for k in range(3):
        a, b, c = (coord[(k + n) % 3] for n in range(3))
        d = (k + 2) % 3
        for o in (1, 2, 3):
            third[k, o].wait_recv()
        total = part3[k, pl.ds(pl.multiple_of(c * 16, 16), 16), :].astype(F32)
        for o in range(3):
            total = total + got3[k, o].astype(F32)
        mine = rows_of(k, (a * 16 + b * 4 + c) * 16, 16)
        c_out[core, mine, :] = total.astype(BF16)
        for o in (1, 3, 2):
            spread[0, k, o] = send(
                c_out.at[core, mine], c_out.at[core, mine],
                send_ag.at[0, k, o - 1], recv_ag.at[0, k, o - 1], (peer(d, o), core),
            )
    for k in range(3):
        a, b = (coord[(k + n) % 3] for n in range(2))
        d = (k + 1) % 3
        for o in (1, 2, 3):
            spread[0, k, o].wait_recv()
        mine = rows_of(k, (a * 4 + b) * 64, 64)
        for o in (1, 3, 2):
            spread[1, k, o] = send(
                c_out.at[core, mine], c_out.at[core, mine],
                send_ag.at[1, k, o - 1], recv_ag.at[1, k, o - 1], (peer(d, o), core),
            )
    across = []
    for k in range(3):
        a = coord[k]
        for o in (1, 2, 3):
            spread[1, k, o].wait_recv()
        mine = rows_of(k, a * 256, 256)
        for o in (1, 3, 2):
            spread[2, k, o] = send(
                c_out.at[core, mine], c_out.at[core, mine],
                send_ag.at[2, k, o - 1], recv_ag.at[2, k, o - 1], (peer(k, o), core),
            )
        across.append(
            send(
                c_out.at[core, mine], c_out.at[core, mine],
                send_cc.at[k, 0], recv_cc.at[k, 0], (me, other),
            )
        )
    for copy in mu3:
        copy.wait_recv()
    mu_copy = send(mu_out.at[core], mu_out.at[core], send_x.at[1], recv_x.at[1], (me, other))
    for o in (1, 3, 2):
        for k in range(3):
            spread[2, k, o].wait_recv()
            got = rows_of(k, lax.rem(coord[k] + 4 - o, 4) * 256, 256)
            across.append(
                send(
                    c_out.at[core, got], c_out.at[core, got],
                    send_cc.at[k, o], recv_cc.at[k, o], (me, other),
                )
            )
    for copy in across:
        copy.wait_recv()
    mu_copy.wait_recv()
    b_copy.wait_recv()
    for copy in started:
        copy.wait_send()


def exchanged(s, mu, b):
    sem = pltpu.SemaphoreType.DMA
    vm = pl.BlockSpec(memory_space=VMEM)
    return pl.pallas_call(
        exchange_kernel,
        out_shape=(
            jax.ShapeDtypeStruct((2, *s.shape), BF16),
            jax.ShapeDtypeStruct((2, 64, 8, 128), F32),
            jax.ShapeDtypeStruct((2, *b.shape), BF16),
        ),
        in_specs=[vm] * 3,
        out_specs=(vm,) * 3,
        scratch_shapes=[
            VMEM((3, 3, 256, B), BF16),
            VMEM((3, 3, 64, B), BF16),
            VMEM((3, 3, 16, B), BF16),
            VMEM((3, 256, B), BF16),
            VMEM((3, 64, B), BF16),
            sem((3, 3, 3)), sem((3, 3, 3)),
            sem((3, 3, 3)), sem((3, 3, 3)),
            sem((3, 4)), sem((3, 4)),
            sem((3, 3)), sem((3, 3)),
            sem((2,)), sem((2,)),
        ],
        compiler_params=pltpu.CompilerParams(
            collective_id=0, has_side_effects=True, vmem_limit_bytes=24 * 2**20
        ),
        name="exchange",
    )(s, mu, b)


PANEL = 32
ROWS_ALL = 196608.0


def split3(v):
    high = v.astype(BF16)
    rest = v - high.astype(F32)
    mid = rest.astype(BF16)
    low = (rest - mid.astype(F32)).astype(BF16)
    return high, mid, low


def nt(a, b):
    return lax.dot_general(a, b, (((1,), (1,)), ((), ())), preferred_element_type=F32)


def nn(a, b):
    return lax.dot_general(a, b, (((1,), (0,)), ((), ())), preferred_element_type=F32)


def factor_panel(a_ref, at):
    low, high = (0, 3) if at < 128 else (1, 4)
    tiles = range(low, high)
    home = at // 128
    groups = PANEL // 8
    rows = [
        [a_ref[at + 8 * g : at + 8 * g + 8, 128 * t : 128 * t + 128] for t in tiles]
        for g in range(groups)
    ]
    line = lax.broadcasted_iota(jnp.int32, (8, 128), 0)
    done = []
    for g in range(groups):
        first = at + 8 * g - 128 * home
        cols = [
            [
                jnp.broadcast_to(rows[t][home - low][:, first + c : first + c + 1], (8, 128))
                for c in range(8)
            ]
            for t in range(g, groups)
        ]
        scale = None
        for j in range(8):
            pivot = jnp.broadcast_to(cols[0][j][j : j + 1, :], (8, 128))
            root = lax.rsqrt(pivot)
            scale = root if scale is None else jnp.where(line >= j, root, scale)
            inverse = root * root
            source = [jnp.broadcast_to(v[j : j + 1, :], (8, 128)) for v in rows[g]]
            heads = [
                jnp.broadcast_to(cols[0][c][j : j + 1, :], (8, 128)) for c in range(j + 1, 8)
            ]
            for t in range(g, groups):
                m = cols[t - g][j] * inverse
                if t == g:
                    m = jnp.where(line > j, m, 0.0)
                for c in range(j + 1, 8):
                    cols[t - g][c] = cols[t - g][c] - m * heads[c - j - 1]
                rows[t] = [v - m * s for v, s in zip(rows[t], source)]
        rows[g] = [v * scale for v in rows[g]]
        done.append(rows[g])
    for g in range(groups):
        for t, v in zip(tiles, done[g]):
            a_ref[at + 8 * g : at + 8 * g + 8, 128 * t : 128 * t + 128] = v
    left = K - at - PANEL
    if left:
        whole = [jnp.concatenate([done[g][n] for g in range(groups)], axis=0) for n in range(3)]
        whole = jnp.concatenate(whole, axis=1)
        high_, mid, low_ = split3(whole)
        right = jnp.concatenate([high_, mid, high_, low_, high_, mid], axis=0)
        side = jnp.concatenate([high_, high_, mid, high_, low_, mid], axis=0)
        side = side[:, : (2 - low) * 128]
        change = lax.dot_general(
            side, right, (((0,), (0,)), ((), ())), preferred_element_type=F32
        )
        skip = at + PANEL - 128 * low
        cols = slice(128 * low, 128 * high)
        a_ref[at + PANEL : K, cols] = a_ref[at + PANEL : K, cols] - change[skip:, :]


def basis_kernel(c_ref, mu_ref, b_ref, x_ref, xb_ref, mean_ref, apart, xb, a_ref, y_ref):
    rows = ROWS_ALL / 64
    for h in range(2):
        for q in range(6):
            at = (h * 6 + q) * 128
            part = mu_ref[h, :, q, :]
            mean = jnp.mean(part, axis=0, keepdims=True)
            mean_ref[:, at : at + 128] = mean
            part = part - mean
            high = part.astype(BF16)
            low = (part - high.astype(F32)).astype(BF16)
            both = jnp.concatenate([high, low], axis=0)
            apart[:128, at : at + 128] = both
            apart[128:, at : at + 128] = both
        xb[128 * h : 128 * h + 128, :] = b_ref[h]

    @pl.loop(0, 3)
    def _(step):
        t = nt(xb[...], apart[:128, :]) * rows
        t = t + pltpu.roll(t, 64, 1)
        high = t.astype(BF16)
        low = (t - high.astype(F32)).astype(BF16)
        t = jnp.concatenate([high, low], axis=1)
        for j in range(NB):
            at = slice(j * B, j * B + B)
            total = nn(t, apart[:, at])
            for i in range(NB):
                o = (j - i) % NB
                left = xb[:, i * B : i * B + B]
                if o < OFFS:
                    r = (i % 3 * OFFS + o) * B
                    total = total + nn(left, c_ref[i // 3, r : r + B, :])
                else:
                    r = (j % 3 * OFFS + NB - o) * B
                    total = total + nt(left, c_ref[j // 3, r : r + B, :])
            total = total * (1.0 / ROWS_ALL)
            high = total.astype(BF16)
            y_ref[:K, at] = high
            y_ref[K:, at] = (total - high.astype(F32)).astype(BF16)

        @pl.when(step == 0)
        def _():
            xb[...] = y_ref[:K, :]

        @pl.when(step > 0)
        def _():
            g = nt(y_ref[...], y_ref[...])
            g = g[:K, :K] + g[K:, K:] + (g[:K, K:] + g[K:, :K])
            a_ref[:, :K] = g
            a_ref[:, K:] = (
                lax.broadcasted_iota(jnp.int32, (K, K), 0)
                == lax.broadcasted_iota(jnp.int32, (K, K), 1)
            ).astype(F32)
            for at in range(0, K, PANEL):
                factor_panel(a_ref, at)
            inverse = a_ref[:, K:]
            inverse = jnp.where(
                lax.broadcasted_iota(jnp.int32, (K, K), 0)
                >= lax.broadcasted_iota(jnp.int32, (K, K), 1),
                inverse, 0.0,
            )
            high = inverse.astype(BF16)
            low = (inverse - high.astype(F32)).astype(BF16)
            for j in range(NB):
                at = slice(j * B, j * B + B)
                x = nn(high, y_ref[:K, at]) + (nn(low, y_ref[:K, at]) + nn(high, y_ref[K:, at]))
                x_ref[:, at] = x
                xb[:, at] = x.astype(BF16)

    xb_ref[...] = xb[...]


def new_basis(c_all, mu_all, b_all):
    vm = pl.BlockSpec(memory_space=VMEM)
    return pl.pallas_call(
        basis_kernel,
        out_shape=(
            jax.ShapeDtypeStruct((K, D), F32),
            jax.ShapeDtypeStruct((K, D), BF16),
            jax.ShapeDtypeStruct((1, D), F32),
        ),
        in_specs=[vm] * 3,
        out_specs=(vm,) * 3,
        scratch_shapes=[
            VMEM((K, D), BF16),
            VMEM((K, D), BF16),
            VMEM((K, 2 * K), F32),
            VMEM((2 * K, D), BF16),
        ],
        compiler_params=pltpu.CompilerParams(vmem_limit_bytes=48 * 2**20),
        name="basis",
    )(c_all, mu_all, b_all)


def project_kernel(e_ref, x_ref, xb_ref, mean_ref, out_ref, basis_ref, xs, off):
    @pl.when(pl.program_id(0) == 0)
    def _():
        core = lax.axis_index("cols")
        own = pl.ds(pl.multiple_of(core * 128, 128), 128)
        xs[:128, :] = xb_ref[own, :]
        xs[128:, :] = xb_ref[pl.ds(pl.multiple_of(128 - core * 128, 128), 128), :]
        basis_ref[...] = x_ref[own, :].T
        parts = [v.astype(F32) for v in split3(jnp.broadcast_to(mean_ref[...], (8, D)))]
        line = lax.broadcasted_iota(jnp.int32, (8, D), 0)
        lines = jnp.where(line == 0, parts[0], jnp.where(line == 1, parts[1], parts[2]))
        lines = jnp.where(line < 3, lines, 0.0).astype(BF16)
        off[...] = jnp.sum(nt(lines, xs[...]), axis=0, keepdims=True)

    for r in range(0, e_ref.shape[0], 256):
        e = e_ref[r : r + 256, :]
        coords = nt(e, xs[...]) - off[...]
        apart = e.astype(F32) - mean_ref[...]
        length = jnp.sum(apart * apart, axis=1, keepdims=True)
        coords = coords * lax.rsqrt(length + 1.0)
        squares = jnp.sum(coords * coords, axis=1, keepdims=True)
        scaled = coords[:, :128] * lax.rsqrt(squares * (1.0 / K) + 0.0001)
        out_ref[r : r + 256, :] = scaled.astype(BF16)


def projected(embeddings, x, xb, mean):
    rows = embeddings.shape[0]
    return pl.pallas_call(
        project_kernel,
        grid=(rows // STEP_ROWS,),
        out_shape=(
            jax.ShapeDtypeStruct((rows, K // 2), BF16),
            jax.ShapeDtypeStruct((D, K // 2), F32),
        ),
        in_specs=[
            pl.BlockSpec((STEP_ROWS, D), lambda s: (s, 0)),
            pl.BlockSpec(memory_space=VMEM),
            pl.BlockSpec(memory_space=VMEM),
            pl.BlockSpec(memory_space=VMEM),
        ],
        out_specs=(
            pl.BlockSpec((STEP_ROWS, K // 2), lambda s: (s, 0)),
            pl.BlockSpec((D, K // 2), lambda s: (0, 0)),
        ),
        scratch_shapes=[VMEM((K, D), BF16), VMEM((1, K), F32)],
        compiler_params=pltpu.CompilerParams(
            vmem_limit_bytes=32 * 2**20, dimension_semantics=("arbitrary",)
        ),
        name="project",
    )(embeddings, x, xb, mean)


def shards(embeddings, start_basis):
    s, mu = local_moment(embeddings)
    c_all, mu_all, b_all = exchanged(s, mu, start_basis.T.astype(BF16))
    return tuple(projected(embeddings, *new_basis(c_all, mu_all, b_all)))


def solution(mesh):
    in_specs = (P("rows", None), P(None, "cols"))
    out_specs = (P("rows", "cols"), P(None, "cols"))
    return jax.shard_map(shards, mesh=mesh, in_specs=in_specs, out_specs=out_specs, check_vma=False)
```

```python
import functools

import jax
import jax.numpy as jnp
from jax import lax
from jax.experimental import pallas as pl
from jax.experimental.pallas import tpu as pltpu
from jax.sharding import PartitionSpec as P

D = 1536
K = 256
B = 256
NB = D // B
OFFS = 4
MESH = pl.DeviceIdType.MESH
VMEM = pltpu.VMEM
F32 = jnp.float32
BF16 = jnp.bfloat16
STRIDES = (1, 4, 16)
STEP_ROWS = 512


def split3(v):
    high = v.astype(BF16)
    rest = v - high.astype(F32)
    mid = rest.astype(BF16)
    low = (rest - mid.astype(F32)).astype(BF16)
    return high, mid, low


def nt(a, b):
    return lax.dot_general(a, b, (((1,), (1,)), ((), ())), preferred_element_type=F32)


def nn(a, b):
    return lax.dot_general(a, b, (((1,), (0,)), ((), ())), preferred_element_type=F32)


def moment_kernel(rows, e_hbm, s_ref, mu_ref, e_ref, turned, sums, outer, sems):
    core = lax.axis_index("cols")
    steps = rows // STEP_ROWS

    def fetch(step):
        at = pl.ds(pl.multiple_of(step * STEP_ROWS, STEP_ROWS), STEP_ROWS)
        return pltpu.make_async_copy(e_hbm.at[at], e_ref.at[at], sems.at[step])

    for step in range(steps):
        fetch(step).start()
    sums[...] = jnp.zeros_like(sums)

    @pl.loop(0, steps)
    def _(step):
        fetch(step).wait()
        start = pl.multiple_of(step * STEP_ROWS, STEP_ROWS)
        for k in range(3):
            i = core * 3 + k
            part = e_ref[pl.ds(start, STEP_ROWS), pl.ds(pl.multiple_of(i * B, B), B)]
            turned[k * B : k * B + B, pl.ds(start, STEP_ROWS)] = part.T
        for q in range(NB):
            at = slice(q * B, q * B + B)
            total = sums[:, at]
            for r in range(0, STEP_ROWS, 16):
                total = total + e_ref[pl.ds(start + r, 16), at].astype(F32)
            sums[:, at] = total

    whole = jnp.sum(sums[...], axis=0, keepdims=True)
    mean = whole * (1.0 / rows)
    sums[0:1, :] = mean
    for k in range(3):
        for half in range(2):
            at = pl.ds(pl.multiple_of((core * 3 + k) * B + half * 128, 128), 128)
            mu_ref[2 * k + half : 2 * k + half + 1, :] = sums[0:1, at]
    mu_ref[6:8, :] = jnp.zeros((2, 128), F32)
    line = lax.broadcasted_iota(jnp.int32, (16, D), 0)

    def lines(v, order):
        parts = split3(jnp.broadcast_to(v, (16, D)))
        out = jnp.zeros((16, D), F32)
        for n, which in enumerate(order):
            out = jnp.where(line == n, parts[which].astype(F32), out)
        return out.astype(BF16)

    outer[:16, :] = lines(whole, (0, 0, 1, 1, 0, 2))
    outer[16:, :] = lines(-mean, (0, 1, 0, 1, 2, 0))

    @pl.loop(0, 3)
    def _(k):
        i = core * 3 + k
        left = outer[:16, pl.ds(pl.multiple_of(i * B, B), B)]
        for o in range(OFFS):
            at = pl.ds(pl.multiple_of(lax.rem(i + o, NB) * B, B), B)
            total = nn(turned[pl.ds(pl.multiple_of(k * B, B), B), :], e_ref[:, at])
            total = total + lax.dot_general(
                left, outer[16:, at], (((0,), (0,)), ((), ())), preferred_element_type=F32
            )
            s_ref[pl.ds(pl.multiple_of((k * OFFS + o) * B, B), B), :] = total.astype(BF16)


def local_moment(embeddings):
    rows = embeddings.shape[0]
    size = 3 * OFFS * B
    return pl.pallas_call(
        functools.partial(moment_kernel, rows),
        out_shape=(
            jax.ShapeDtypeStruct((size, B), BF16),
            jax.ShapeDtypeStruct((8, 128), F32),
        ),
        in_specs=[pl.BlockSpec(memory_space=pltpu.HBM)],
        out_specs=(pl.BlockSpec(memory_space=VMEM),) * 2,
        scratch_shapes=[
            VMEM((rows, D), BF16),
            VMEM((3 * B, rows), BF16),
            VMEM((16, D), F32),
            VMEM((32, D), BF16),
            pltpu.SemaphoreType.DMA((rows // STEP_ROWS,)),
        ],
        compiler_params=pltpu.CompilerParams(vmem_limit_bytes=56 * 2**20),
        name="moment",
    )(embeddings)


def exchange_kernel(
    s_ref, mu_ref, b_ref,
    c_out, mu_out, b_out,
    got1, got2, got3, part2, part3,
    send_rs, recv_rs, send_ag, recv_ag, send_cc, recv_cc, send_mu, recv_mu, send_x, recv_x,
):
    me = lax.axis_index("rows")
    core = lax.axis_index("cols")
    other = 1 - core
    coord = [lax.rem(me // s, 4) for s in STRIDES]

    def peer(dim, o):
        return me + (lax.rem(coord[dim] + o, 4) - coord[dim]) * STRIDES[dim]

    barrier = pltpu.get_barrier_semaphore()
    for dim in range(3):
        for o in (1, 2, 3):
            pl.semaphore_signal(barrier, inc=1, device_id=(peer(dim, o), core), device_id_type=MESH)
    pl.semaphore_signal(barrier, inc=1, device_id=(me, other), device_id_type=MESH)
    pl.semaphore_wait(barrier, 10)

    started = []

    def send(src, dst, send_sem, recv_sem, to):
        copy = pltpu.make_async_remote_copy(
            src_ref=src, dst_ref=dst, send_sem=send_sem, recv_sem=recv_sem,
            device_id=to, device_id_type=MESH,
        )
        copy.start()
        started.append(copy)
        return copy

    def rows_of(k, start, size):
        return pl.ds(pl.multiple_of(k * 1024 + start, 16), size)

    first = {}
    for o in (1, 3, 2):
        for k in range(3):
            to = lax.rem(coord[k] + o, 4)
            first[k, o] = send(
                s_ref.at[rows_of(k, to * 256, 256)], got1.at[k, o - 1],
                send_rs.at[0, k, o - 1], recv_rs.at[0, k, o - 1], (peer(k, o), core),
            )
    mu_out[core, me] = mu_ref[...]
    mu1 = [
        send(
            mu_ref, mu_out.at[core, me], send_mu.at[0, o - 1], recv_mu.at[0, o - 1],
            (peer(0, o), core),
        )
        for o in (1, 2, 3)
    ]
    b_copy = send(b_ref, b_out.at[core], send_x.at[0], recv_x.at[0], (me, other))
    b_out[core] = b_ref[...]

    second = {}
    for k in range(3):
        for o in (1, 2, 3):
            first[k, o].wait_recv()
        total = s_ref[rows_of(k, coord[k] * 256, 256), :].astype(F32)
        for o in range(3):
            total = total + got1[k, o].astype(F32)
        part2[k] = total.astype(BF16)
        d = (k + 1) % 3
        for o in (1, 3, 2):
            to = lax.rem(coord[d] + o, 4)
            second[k, o] = send(
                part2.at[k, pl.ds(pl.multiple_of(to * 64, 16), 64)], got2.at[k, o - 1],
                send_rs.at[1, k, o - 1], recv_rs.at[1, k, o - 1], (peer(d, o), core),
            )
    for copy in mu1:
        copy.wait_recv()
    line = pl.multiple_of(me // 4 * 4, 4)
    mu2 = [
        send(
            mu_out.at[core, pl.ds(line, 4)], mu_out.at[core, pl.ds(line, 4)],
            send_mu.at[1, o - 1], recv_mu.at[1, o - 1], (peer(1, o), core),
        )
        for o in (1, 2, 3)
    ]
    third = {}
    for k in range(3):
        d = (k + 1) % 3
        for o in (1, 2, 3):
            second[k, o].wait_recv()
        total = part2[k, pl.ds(pl.multiple_of(coord[d] * 64, 16), 64), :].astype(F32)
        for o in range(3):
            total = total + got2[k, o].astype(F32)
        part3[k] = total.astype(BF16)
        d = (k + 2) % 3
        for o in (1, 3, 2):
            to = lax.rem(coord[d] + o, 4)
            third[k, o] = send(
                part3.at[k, pl.ds(pl.multiple_of(to * 16, 16), 16)], got3.at[k, o - 1],
                send_rs.at[2, k, o - 1], recv_rs.at[2, k, o - 1], (peer(d, o), core),
            )
    for copy in mu2:
        copy.wait_recv()
    plane = pl.multiple_of(me // 16 * 16, 16)
    mu3 = [
        send(
            mu_out.at[core, pl.ds(plane, 16)], mu_out.at[core, pl.ds(plane, 16)],
            send_mu.at[2, o - 1], recv_mu.at[2, o - 1], (peer(2, o), core),
        )
        for o in (1, 2, 3)
    ]
    spread = {}
    for k in range(3):
        a, b, c = (coord[(k + n) % 3] for n in range(3))
        d = (k + 2) % 3
        for o in (1, 2, 3):
            third[k, o].wait_recv()
        total = part3[k, pl.ds(pl.multiple_of(c * 16, 16), 16), :].astype(F32)
        for o in range(3):
            total = total + got3[k, o].astype(F32)
        mine = rows_of(k, (a * 16 + b * 4 + c) * 16, 16)
        c_out[core, mine, :] = total.astype(BF16)
        for o in (1, 3, 2):
            spread[0, k, o] = send(
                c_out.at[core, mine], c_out.at[core, mine],
                send_ag.at[0, k, o - 1], recv_ag.at[0, k, o - 1], (peer(d, o), core),
            )
    for k in range(3):
        a, b = (coord[(k + n) % 3] for n in range(2))
        d = (k + 1) % 3
        for o in (1, 2, 3):
            spread[0, k, o].wait_recv()
        mine = rows_of(k, (a * 4 + b) * 64, 64)
        for o in (1, 3, 2):
            spread[1, k, o] = send(
                c_out.at[core, mine], c_out.at[core, mine],
                send_ag.at[1, k, o - 1], recv_ag.at[1, k, o - 1], (peer(d, o), core),
            )
    across = []
    for k in range(3):
        a = coord[k]
        for o in (1, 2, 3):
            spread[1, k, o].wait_recv()
        mine = rows_of(k, a * 256, 256)
        for o in (1, 3, 2):
            spread[2, k, o] = send(
                c_out.at[core, mine], c_out.at[core, mine],
                send_ag.at[2, k, o - 1], recv_ag.at[2, k, o - 1], (peer(k, o), core),
            )
        across.append(
            send(
                c_out.at[core, mine], c_out.at[core, mine],
                send_cc.at[k, 0], recv_cc.at[k, 0], (me, other),
            )
        )
    for copy in mu3:
        copy.wait_recv()
    mu_copy = send(mu_out.at[core], mu_out.at[core], send_x.at[1], recv_x.at[1], (me, other))
    for o in (1, 3, 2):
        for k in range(3):
            spread[2, k, o].wait_recv()
            got = rows_of(k, lax.rem(coord[k] + 4 - o, 4) * 256, 256)
            across.append(
                send(
                    c_out.at[core, got], c_out.at[core, got],
                    send_cc.at[k, o], recv_cc.at[k, o], (me, other),
                )
            )
    for copy in across:
        copy.wait_recv()
    mu_copy.wait_recv()
    b_copy.wait_recv()
    for copy in started:
        copy.wait_send()


def exchanged(s, mu, b):
    sem = pltpu.SemaphoreType.DMA
    vm = pl.BlockSpec(memory_space=VMEM)
    return pl.pallas_call(
        exchange_kernel,
        out_shape=(
            jax.ShapeDtypeStruct((2, *s.shape), BF16),
            jax.ShapeDtypeStruct((2, 64, 8, 128), F32),
            jax.ShapeDtypeStruct((2, *b.shape), BF16),
        ),
        in_specs=[vm] * 3,
        out_specs=(vm,) * 3,
        scratch_shapes=[
            VMEM((3, 3, 256, B), BF16),
            VMEM((3, 3, 64, B), BF16),
            VMEM((3, 3, 16, B), BF16),
            VMEM((3, 256, B), BF16),
            VMEM((3, 64, B), BF16),
            sem((3, 3, 3)), sem((3, 3, 3)),
            sem((3, 3, 3)), sem((3, 3, 3)),
            sem((3, 4)), sem((3, 4)),
            sem((3, 3)), sem((3, 3)),
            sem((2,)), sem((2,)),
        ],
        compiler_params=pltpu.CompilerParams(
            collective_id=0, has_side_effects=True, vmem_limit_bytes=24 * 2**20
        ),
        name="exchange",
    )(s, mu, b)


PANEL = 32
ROWS_ALL = 196608.0


def factor_panel(a_ref, at):
    low, high = (0, 3) if at < 128 else (1, 4)
    tiles = range(low, high)
    home = at // 128
    groups = PANEL // 8
    rows = [
        [a_ref[at + 8 * g : at + 8 * g + 8, 128 * t : 128 * t + 128] for t in tiles]
        for g in range(groups)
    ]
    line = lax.broadcasted_iota(jnp.int32, (8, 128), 0)
    done = []
    for g in range(groups):
        first = at + 8 * g - 128 * home
        cols = [
            [
                jnp.broadcast_to(rows[t][home - low][:, first + c : first + c + 1], (8, 128))
                for c in range(8)
            ]
            for t in range(g, groups)
        ]
        scale = None
        for j in range(8):
            pivot = jnp.broadcast_to(cols[0][j][j : j + 1, :], (8, 128))
            root = lax.rsqrt(pivot)
            scale = root if scale is None else jnp.where(line >= j, root, scale)
            inverse = root * root
            source = [jnp.broadcast_to(v[j : j + 1, :], (8, 128)) for v in rows[g]]
            heads = [
                jnp.broadcast_to(cols[0][c][j : j + 1, :], (8, 128)) for c in range(j + 1, 8)
            ]
            for t in range(g, groups):
                m = cols[t - g][j] * inverse
                if t == g:
                    m = jnp.where(line > j, m, 0.0)
                for c in range(j + 1, 8):
                    cols[t - g][c] = cols[t - g][c] - m * heads[c - j - 1]
                rows[t] = [v - m * s for v, s in zip(rows[t], source)]
        rows[g] = [v * scale for v in rows[g]]
        done.append(rows[g])
    for g in range(groups):
        for t, v in zip(tiles, done[g]):
            a_ref[at + 8 * g : at + 8 * g + 8, 128 * t : 128 * t + 128] = v
    left = K - at - PANEL
    if left:
        whole = [jnp.concatenate([done[g][n] for g in range(groups)], axis=0) for n in range(3)]
        whole = jnp.concatenate(whole, axis=1)
        high_, mid, low_ = split3(whole)
        right = jnp.concatenate([high_, mid, high_, low_, high_, mid], axis=0)
        side = jnp.concatenate([high_, high_, mid, high_, low_, mid], axis=0)
        side = side[:, : (2 - low) * 128]
        change = lax.dot_general(
            side, right, (((0,), (0,)), ((), ())), preferred_element_type=F32
        )
        skip = at + PANEL - 128 * low
        cols = slice(128 * low, 128 * high)
        a_ref[at + PANEL : K, cols] = a_ref[at + PANEL : K, cols] - change[skip:, :]


def basis_kernel(c_ref, mu_ref, b_ref, x_ref, xb_ref, mean_ref, apart, xb, a_ref, y_ref):
    rows = ROWS_ALL / 64
    for h in range(2):
        for q in range(6):
            at = (h * 6 + q) * 128
            part = mu_ref[h, :, q, :]
            mean = jnp.mean(part, axis=0, keepdims=True)
            mean_ref[:, at : at + 128] = mean
            part = part - mean
            high = part.astype(BF16)
            low = (part - high.astype(F32)).astype(BF16)
            both = jnp.concatenate([high, low], axis=0)
            apart[:128, at : at + 128] = both
            apart[128:, at : at + 128] = both
        xb[128 * h : 128 * h + 128, :] = b_ref[h]

    @pl.loop(0, 3)
    def _(step):
        t = nt(xb[...], apart[:128, :]) * rows
        t = t + pltpu.roll(t, 64, 1)
        high = t.astype(BF16)
        low = (t - high.astype(F32)).astype(BF16)
        t = jnp.concatenate([high, low], axis=1)
        for j in range(NB):
            at = slice(j * B, j * B + B)
            total = nn(t, apart[:, at])
            for i in range(NB):
                o = (j - i) % NB
                left = xb[:, i * B : i * B + B]
                if o < OFFS:
                    r = (i % 3 * OFFS + o) * B
                    total = total + nn(left, c_ref[i // 3, r : r + B, :])
                else:
                    r = (j % 3 * OFFS + NB - o) * B
                    total = total + nt(left, c_ref[j // 3, r : r + B, :])
            total = total * (1.0 / ROWS_ALL)
            high = total.astype(BF16)
            y_ref[:K, at] = high
            y_ref[K:, at] = (total - high.astype(F32)).astype(BF16)

        @pl.when(step == 0)
        def _():
            xb[...] = y_ref[:K, :]

        @pl.when(step > 0)
        def _():
            g = nt(y_ref[...], y_ref[...])
            g = g[:K, :K] + g[K:, K:] + (g[:K, K:] + g[K:, :K])
            a_ref[:, :K] = g
            a_ref[:, K:] = (
                lax.broadcasted_iota(jnp.int32, (K, K), 0)
                == lax.broadcasted_iota(jnp.int32, (K, K), 1)
            ).astype(F32)
            for at in range(0, K, PANEL):
                factor_panel(a_ref, at)
            inverse = a_ref[:, K:]
            inverse = jnp.where(
                lax.broadcasted_iota(jnp.int32, (K, K), 0)
                >= lax.broadcasted_iota(jnp.int32, (K, K), 1),
                inverse, 0.0,
            )
            high = inverse.astype(BF16)
            low = (inverse - high.astype(F32)).astype(BF16)
            for j in range(NB):
                at = slice(j * B, j * B + B)
                x = nn(high, y_ref[:K, at]) + (nn(low, y_ref[:K, at]) + nn(high, y_ref[K:, at]))
                x_ref[:, at] = x
                xb[:, at] = x.astype(BF16)

    xb_ref[...] = xb[...]


def new_basis(c_all, mu_all, b_all):
    vm = pl.BlockSpec(memory_space=VMEM)
    return pl.pallas_call(
        basis_kernel,
        out_shape=(
            jax.ShapeDtypeStruct((K, D), F32),
            jax.ShapeDtypeStruct((K, D), BF16),
            jax.ShapeDtypeStruct((1, D), F32),
        ),
        in_specs=[vm] * 3,
        out_specs=(vm,) * 3,
        scratch_shapes=[
            VMEM((K, D), BF16),
            VMEM((K, D), BF16),
            VMEM((K, 2 * K), F32),
            VMEM((2 * K, D), BF16),
        ],
        compiler_params=pltpu.CompilerParams(vmem_limit_bytes=20 * 2**20),
        name="basis",
    )(c_all, mu_all, b_all)


def project_kernel(e_ref, x_ref, xb_ref, mean_ref, out_ref, basis_ref, xs, off):
    @pl.when(pl.program_id(0) == 0)
    def _():
        core = lax.axis_index("cols")
        own = pl.ds(pl.multiple_of(core * 128, 128), 128)
        xs[:128, :] = xb_ref[own, :]
        xs[128:, :] = xb_ref[pl.ds(pl.multiple_of(128 - core * 128, 128), 128), :]
        basis_ref[...] = x_ref[own, :].T
        parts = [v.astype(F32) for v in split3(jnp.broadcast_to(mean_ref[...], (8, D)))]
        line = lax.broadcasted_iota(jnp.int32, (8, D), 0)
        lines = jnp.where(line == 0, parts[0], jnp.where(line == 1, parts[1], parts[2]))
        lines = jnp.where(line < 3, lines, 0.0).astype(BF16)
        off[...] = jnp.sum(nt(lines, xs[...]), axis=0, keepdims=True)

    for r in range(0, e_ref.shape[0], 256):
        e = e_ref[r : r + 256, :]
        coords = nt(e, xs[...]) - off[...]
        apart = e.astype(F32) - mean_ref[...]
        length = jnp.sum(apart * apart, axis=1, keepdims=True)
        coords = coords * lax.rsqrt(length + 1.0)
        squares = jnp.sum(coords * coords, axis=1, keepdims=True)
        scaled = coords[:, :128] * lax.rsqrt(squares * (1.0 / K) + 0.0001)
        out_ref[r : r + 256, :] = scaled.astype(BF16)


def projected(embeddings, x, xb, mean):
    rows = embeddings.shape[0]
    return pl.pallas_call(
        project_kernel,
        grid=(rows // STEP_ROWS,),
        out_shape=(
            jax.ShapeDtypeStruct((rows, K // 2), BF16),
            jax.ShapeDtypeStruct((D, K // 2), F32),
        ),
        in_specs=[
            pl.BlockSpec((STEP_ROWS, D), lambda s: (s, 0)),
            pl.BlockSpec(memory_space=VMEM),
            pl.BlockSpec(memory_space=VMEM),
            pl.BlockSpec(memory_space=VMEM),
        ],
        out_specs=(
            pl.BlockSpec((STEP_ROWS, K // 2), lambda s: (s, 0)),
            pl.BlockSpec((D, K // 2), lambda s: (0, 0)),
        ),
        scratch_shapes=[VMEM((K, D), BF16), VMEM((1, K), F32)],
        compiler_params=pltpu.CompilerParams(
            vmem_limit_bytes=56 * 2**20, dimension_semantics=("arbitrary",)
        ),
        name="project",
    )(embeddings, x, xb, mean)


def shards(embeddings, start_basis):
    s, mu = local_moment(embeddings)
    c_all, mu_all, b_all = exchanged(s, mu, start_basis.T.astype(BF16))
    return tuple(projected(embeddings, *new_basis(c_all, mu_all, b_all)))


def solution(mesh):
    in_specs = (P("rows", None), P(None, "cols"))
    out_specs = (P("rows", "cols"), P(None, "cols"))
    return jax.shard_map(shards, mesh=mesh, in_specs=in_specs, out_specs=out_specs, check_vma=False)
```

```python
import functools

import jax
import jax.numpy as jnp
from jax import lax
from jax.experimental import pallas as pl
from jax.experimental.pallas import tpu as pltpu
from jax.sharding import PartitionSpec as P

D = 1536
K = 256
B = 256
NB = D // B
OFFS = 4
MESH = pl.DeviceIdType.MESH
VMEM = pltpu.VMEM
F32 = jnp.float32
BF16 = jnp.bfloat16
STRIDES = (1, 4, 16)
STEP_ROWS = 512


def split3(v):
    high = v.astype(BF16)
    rest = v - high.astype(F32)
    mid = rest.astype(BF16)
    low = (rest - mid.astype(F32)).astype(BF16)
    return high, mid, low


def nt(a, b):
    return lax.dot_general(a, b, (((1,), (1,)), ((), ())), preferred_element_type=F32)


def nn(a, b):
    return lax.dot_general(a, b, (((1,), (0,)), ((), ())), preferred_element_type=F32)


def gather_kernel(
    rows, e_hbm, b_ref,
    c_out, mu_out, b_out, length_out,
    e_ref, turned, s_ref, mu_ref, sums, outer,
    got1, got2, got3, part2, part3, fetched,
    send_rs, recv_rs, send_ag, recv_ag, send_cc, recv_cc, send_mu, recv_mu, send_x, recv_x,
):
    me = lax.axis_index("rows")
    core = lax.axis_index("cols")
    other = 1 - core
    coord = [lax.rem(me // s, 4) for s in STRIDES]
    steps = rows // STEP_ROWS

    def fetch(step):
        at = pl.ds(pl.multiple_of(step * STEP_ROWS, STEP_ROWS), STEP_ROWS)
        return pltpu.make_async_copy(e_hbm.at[at], e_ref.at[at], fetched.at[step])

    for step in range(steps):
        fetch(step).start()

    def peer(dim, o):
        return me + (lax.rem(coord[dim] + o, 4) - coord[dim]) * STRIDES[dim]

    barrier = pltpu.get_barrier_semaphore()
    for dim in range(3):
        for o in (1, 2, 3):
            pl.semaphore_signal(barrier, inc=1, device_id=(peer(dim, o), core), device_id_type=MESH)
    pl.semaphore_signal(barrier, inc=1, device_id=(me, other), device_id_type=MESH)

    sums[...] = jnp.zeros_like(sums)

    @pl.loop(0, steps)
    def _(step):
        fetch(step).wait()
        start = pl.multiple_of(step * STEP_ROWS, STEP_ROWS)
        for k in range(3):
            i = core * 3 + k
            part = e_ref[pl.ds(start, STEP_ROWS), pl.ds(pl.multiple_of(i * B, B), B)]
            turned[k * B : k * B + B, pl.ds(start, STEP_ROWS)] = part.T
        for q in range(NB):
            at = slice(q * B, q * B + B)
            total = sums[:, at]
            for r in range(0, STEP_ROWS, 16):
                total = total + e_ref[pl.ds(start + r, 16), at].astype(F32)
            sums[:, at] = total

    whole = jnp.sum(sums[...], axis=0, keepdims=True)
    mean = whole * (1.0 / rows)
    sums[0:1, :] = mean
    for k in range(3):
        for half in range(2):
            at = pl.ds(pl.multiple_of((core * 3 + k) * B + half * 128, 128), 128)
            mu_ref[2 * k + half : 2 * k + half + 1, :] = sums[0:1, at]
    mu_ref[6:8, :] = jnp.zeros((2, 128), F32)
    mu_out[core, me] = mu_ref[...]
    b_out[core] = b_ref[...]

    started = []

    def send(src, dst, send_sem, recv_sem, to):
        copy = pltpu.make_async_remote_copy(
            src_ref=src, dst_ref=dst, send_sem=send_sem, recv_sem=recv_sem,
            device_id=to, device_id_type=MESH,
        )
        copy.start()
        started.append(copy)
        return copy

    def rows_of(k, start, size):
        return pl.ds(pl.multiple_of(k * 1024 + start, 16), size)

    pl.semaphore_wait(barrier, 10)

    def send_means(n, at):
        return [
            send(
                mu_out.at[core, at], mu_out.at[core, at],
                send_mu.at[n, o - 1], recv_mu.at[n, o - 1], (peer(n, o), core),
            )
            for o in (1, 3, 2)
        ]

    means = send_means(0, pl.ds(me, 1))
    b_copy = send(b_ref, b_out.at[core], send_x.at[0], recv_x.at[0], (me, other))

    line = lax.broadcasted_iota(jnp.int32, (16, D), 0)

    def lines(v, order):
        parts = split3(jnp.broadcast_to(v, (16, D)))
        out = jnp.zeros((16, D), F32)
        for n, which in enumerate(order):
            out = jnp.where(line == n, parts[which].astype(F32), out)
        return out.astype(BF16)

    outer[:16, :] = lines(whole, (0, 0, 1, 1, 0, 2))
    outer[16:, :] = lines(-mean, (0, 1, 0, 1, 2, 0))

    first = {}
    for k in range(3):
        i = core * 3 + k
        left = outer[:16, pl.ds(pl.multiple_of(i * B, B), B)]

        @pl.loop(0, OFFS)
        def _(o):
            at = pl.ds(pl.multiple_of(lax.rem(i + o, NB) * B, B), B)
            total = nn(turned[k * B : k * B + B, :], e_ref[:, at])
            total = total + lax.dot_general(
                left, outer[16:, at], (((0,), (0,)), ((), ())), preferred_element_type=F32
            )
            s_ref[pl.ds(pl.multiple_of((k * OFFS + o) * B, B), B), :] = total.astype(BF16)

        for o in (1, 3, 2):
            to = lax.rem(coord[k] + o, 4)
            first[k, o] = send(
                s_ref.at[rows_of(k, to * 256, 256)], got1.at[k, o - 1],
                send_rs.at[0, k, o - 1], recv_rs.at[0, k, o - 1], (peer(k, o), core),
            )
        for copy in means:
            copy.wait_recv()
        if k == 0:
            means = send_means(1, pl.ds(pl.multiple_of(me // 4 * 4, 4), 4))
        elif k == 1:
            means = send_means(2, pl.ds(pl.multiple_of(me // 16 * 16, 16), 16))
    mu_copy = send(mu_out.at[core], mu_out.at[core], send_x.at[1], recv_x.at[1], (me, other))
    mu_copy.wait_recv()

    for h in range(2):
        for q in range(6):
            at = (h * 6 + q) * 128
            sums[0:1, at : at + 128] = jnp.mean(mu_out[h, :, q, :], axis=0, keepdims=True)

    @pl.loop(0, rows // 64)
    def _(n):
        at = pl.ds(pl.multiple_of(n * 64, 64), 64)
        apart = e_ref[at, :].astype(F32) - sums[0:1, :]
        length_out[at, :] = lax.rsqrt(jnp.sum(apart * apart, axis=1, keepdims=True) + 1.0)

    second = {}
    for k in range(3):
        for o in (1, 2, 3):
            first[k, o].wait_recv()
        total = s_ref[rows_of(k, coord[k] * 256, 256), :].astype(F32)
        for o in range(3):
            total = total + got1[k, o].astype(F32)
        part2[k] = total.astype(BF16)
        d = (k + 1) % 3
        for o in (1, 3, 2):
            to = lax.rem(coord[d] + o, 4)
            second[k, o] = send(
                part2.at[k, pl.ds(pl.multiple_of(to * 64, 16), 64)], got2.at[k, o - 1],
                send_rs.at[1, k, o - 1], recv_rs.at[1, k, o - 1], (peer(d, o), core),
            )
    third = {}
    for k in range(3):
        d = (k + 1) % 3
        for o in (1, 2, 3):
            second[k, o].wait_recv()
        total = part2[k, pl.ds(pl.multiple_of(coord[d] * 64, 16), 64), :].astype(F32)
        for o in range(3):
            total = total + got2[k, o].astype(F32)
        part3[k] = total.astype(BF16)
        d = (k + 2) % 3
        for o in (1, 3, 2):
            to = lax.rem(coord[d] + o, 4)
            third[k, o] = send(
                part3.at[k, pl.ds(pl.multiple_of(to * 16, 16), 16)], got3.at[k, o - 1],
                send_rs.at[2, k, o - 1], recv_rs.at[2, k, o - 1], (peer(d, o), core),
            )
    spread = {}
    for k in range(3):
        a, b, c = (coord[(k + n) % 3] for n in range(3))
        d = (k + 2) % 3
        for o in (1, 2, 3):
            third[k, o].wait_recv()
        total = part3[k, pl.ds(pl.multiple_of(c * 16, 16), 16), :].astype(F32)
        for o in range(3):
            total = total + got3[k, o].astype(F32)
        mine = rows_of(k, (a * 16 + b * 4 + c) * 16, 16)
        c_out[core, mine, :] = total.astype(BF16)
        for o in (1, 3, 2):
            spread[0, k, o] = send(
                c_out.at[core, mine], c_out.at[core, mine],
                send_ag.at[0, k, o - 1], recv_ag.at[0, k, o - 1], (peer(d, o), core),
            )
    for k in range(3):
        a, b = (coord[(k + n) % 3] for n in range(2))
        d = (k + 1) % 3
        for o in (1, 2, 3):
            spread[0, k, o].wait_recv()
        mine = rows_of(k, (a * 4 + b) * 64, 64)
        for o in (1, 3, 2):
            spread[1, k, o] = send(
                c_out.at[core, mine], c_out.at[core, mine],
                send_ag.at[1, k, o - 1], recv_ag.at[1, k, o - 1], (peer(d, o), core),
            )
    across = []
    for k in range(3):
        a = coord[k]
        for o in (1, 2, 3):
            spread[1, k, o].wait_recv()
        mine = rows_of(k, a * 256, 256)
        for o in (1, 3, 2):
            spread[2, k, o] = send(
                c_out.at[core, mine], c_out.at[core, mine],
                send_ag.at[2, k, o - 1], recv_ag.at[2, k, o - 1], (peer(k, o), core),
            )
        across.append(
            send(
                c_out.at[core, mine], c_out.at[core, mine],
                send_cc.at[k, 0], recv_cc.at[k, 0], (me, other),
            )
        )
    for o in (1, 3, 2):
        for k in range(3):
            spread[2, k, o].wait_recv()
            got = rows_of(k, lax.rem(coord[k] + 4 - o, 4) * 256, 256)
            across.append(
                send(
                    c_out.at[core, got], c_out.at[core, got],
                    send_cc.at[k, o], recv_cc.at[k, o], (me, other),
                )
            )
    for copy in across:
        copy.wait_recv()
    b_copy.wait_recv()
    for copy in started:
        copy.wait_send()


def gathered(embeddings, b):
    rows = embeddings.shape[0]
    size = 3 * OFFS * B
    sem = pltpu.SemaphoreType.DMA
    vm = pl.BlockSpec(memory_space=VMEM)
    return pl.pallas_call(
        functools.partial(gather_kernel, rows),
        out_shape=(
            jax.ShapeDtypeStruct((2, size, B), BF16),
            jax.ShapeDtypeStruct((2, 64, 8, 128), F32),
            jax.ShapeDtypeStruct((2, *b.shape), BF16),
            jax.ShapeDtypeStruct((rows, 1), F32),
        ),
        in_specs=[pl.BlockSpec(memory_space=pltpu.HBM), vm],
        out_specs=(vm,) * 4,
        scratch_shapes=[
            VMEM((rows, D), BF16),
            VMEM((3 * B, rows), BF16),
            VMEM((size, B), BF16),
            VMEM((8, 128), F32),
            VMEM((16, D), F32),
            VMEM((32, D), BF16),
            VMEM((3, 3, 256, B), BF16),
            VMEM((3, 3, 64, B), BF16),
            VMEM((3, 3, 16, B), BF16),
            VMEM((3, 256, B), BF16),
            VMEM((3, 64, B), BF16),
            sem((rows // STEP_ROWS,)),
            sem((3, 3, 3)), sem((3, 3, 3)),
            sem((3, 3, 3)), sem((3, 3, 3)),
            sem((3, 4)), sem((3, 4)),
            sem((3, 3)), sem((3, 3)),
            sem((2,)), sem((2,)),
        ],
        compiler_params=pltpu.CompilerParams(
            collective_id=0, has_side_effects=True, vmem_limit_bytes=46 * 2**20
        ),
        name="gather",
    )(embeddings, b)


PANEL = 32
ROWS_ALL = 196608.0


def factor_panel(a_ref, at):
    low, high = (0, 3) if at < 128 else (1, 4)
    tiles = range(low, high)
    home = at // 128
    groups = PANEL // 8
    rows = [
        [a_ref[at + 8 * g : at + 8 * g + 8, 128 * t : 128 * t + 128] for t in tiles]
        for g in range(groups)
    ]
    line = lax.broadcasted_iota(jnp.int32, (8, 128), 0)
    done = []
    for g in range(groups):
        first = at + 8 * g - 128 * home
        cols = [
            [
                jnp.broadcast_to(rows[t][home - low][:, first + c : first + c + 1], (8, 128))
                for c in range(8)
            ]
            for t in range(g, groups)
        ]
        scale = None
        for j in range(8):
            pivot = jnp.broadcast_to(cols[0][j][j : j + 1, :], (8, 128))
            root = lax.rsqrt(pivot)
            scale = root if scale is None else jnp.where(line >= j, root, scale)
            inverse = root * root
            source = [jnp.broadcast_to(v[j : j + 1, :], (8, 128)) for v in rows[g]]
            heads = [
                jnp.broadcast_to(cols[0][c][j : j + 1, :], (8, 128)) for c in range(j + 1, 8)
            ]
            for t in range(g, groups):
                m = cols[t - g][j] * inverse
                if t == g:
                    m = jnp.where(line > j, m, 0.0)
                for c in range(j + 1, 8):
                    cols[t - g][c] = cols[t - g][c] - m * heads[c - j - 1]
                rows[t] = [v - m * s for v, s in zip(rows[t], source)]
        rows[g] = [v * scale for v in rows[g]]
        done.append(rows[g])
    for g in range(groups):
        for t, v in zip(tiles, done[g]):
            a_ref[at + 8 * g : at + 8 * g + 8, 128 * t : 128 * t + 128] = v
    left = K - at - PANEL
    if left:
        whole = [jnp.concatenate([done[g][n] for g in range(groups)], axis=0) for n in range(3)]
        whole = jnp.concatenate(whole, axis=1)
        high_, mid, low_ = split3(whole)
        right = jnp.concatenate([high_, mid, high_, low_, high_, mid], axis=0)
        side = jnp.concatenate([high_, high_, mid, high_, low_, mid], axis=0)
        side = side[:, : (2 - low) * 128]
        change = lax.dot_general(
            side, right, (((0,), (0,)), ((), ())), preferred_element_type=F32
        )
        skip = at + PANEL - 128 * low
        cols = slice(128 * low, 128 * high)
        a_ref[at + PANEL : K, cols] = a_ref[at + PANEL : K, cols] - change[skip:, :]


def finish_kernel(
    e_hbm, c_ref, mu_ref, b_ref, length_ref, out_hbm, basis_hbm,
    e_ref, x_ref, mean_ref, apart, xb, a_ref, y_ref, out_ref, basis_ref, fetched, written,
):
    rows = e_ref.shape[0]
    steps = rows // STEP_ROWS

    def fetch(step):
        at = pl.ds(pl.multiple_of(step * STEP_ROWS, STEP_ROWS), STEP_ROWS)
        return pltpu.make_async_copy(e_hbm.at[at], e_ref.at[at], fetched.at[step])

    for step in range(steps):
        fetch(step).start()
    for h in range(2):
        for q in range(6):
            at = (h * 6 + q) * 128
            part = mu_ref[h, :, q, :]
            mean = jnp.mean(part, axis=0, keepdims=True)
            mean_ref[:, at : at + 128] = mean
            part = part - mean
            high = part.astype(BF16)
            low = (part - high.astype(F32)).astype(BF16)
            both = jnp.concatenate([high, low], axis=0)
            apart[:128, at : at + 128] = both
            apart[128:, at : at + 128] = both
        xb[128 * h : 128 * h + 128, :] = b_ref[h]

    @pl.loop(0, 3)
    def _(step):
        t = nt(xb[...], apart[:128, :]) * float(rows)
        t = t + pltpu.roll(t, 64, 1)
        high = t.astype(BF16)
        low = (t - high.astype(F32)).astype(BF16)
        t = jnp.concatenate([high, low], axis=1)
        for j in range(NB):
            at = slice(j * B, j * B + B)
            total = nn(t, apart[:, at])
            for i in range(NB):
                o = (j - i) % NB
                left = xb[:, i * B : i * B + B]
                if o < OFFS:
                    r = (i % 3 * OFFS + o) * B
                    total = total + nn(left, c_ref[i // 3, r : r + B, :])
                else:
                    r = (j % 3 * OFFS + NB - o) * B
                    total = total + nt(left, c_ref[j // 3, r : r + B, :])
            total = total * (1.0 / ROWS_ALL)
            high = total.astype(BF16)
            y_ref[:K, at] = high
            y_ref[K:, at] = (total - high.astype(F32)).astype(BF16)

        @pl.when(step == 0)
        def _():
            xb[...] = y_ref[:K, :]

        @pl.when(step > 0)
        def _():
            g = nt(y_ref[...], y_ref[...])
            g = g[:K, :K] + g[K:, K:] + (g[:K, K:] + g[K:, :K])
            a_ref[:, :K] = g
            a_ref[:, K:] = (
                lax.broadcasted_iota(jnp.int32, (K, K), 0)
                == lax.broadcasted_iota(jnp.int32, (K, K), 1)
            ).astype(F32)
            for at in range(0, K, PANEL):
                factor_panel(a_ref, at)
            inverse = a_ref[:, K:]
            inverse = jnp.where(
                lax.broadcasted_iota(jnp.int32, (K, K), 0)
                >= lax.broadcasted_iota(jnp.int32, (K, K), 1),
                inverse, 0.0,
            )
            high = inverse.astype(BF16)
            low = (inverse - high.astype(F32)).astype(BF16)
            for j in range(NB):
                at = slice(j * B, j * B + B)
                x = nn(high, y_ref[:K, at]) + (nn(low, y_ref[:K, at]) + nn(high, y_ref[K:, at]))
                x_ref[:, at] = x
                xb[:, at] = x.astype(BF16)

    core = lax.axis_index("cols")
    own = pl.ds(pl.multiple_of(core * 128, 128), 128)
    basis_ref[...] = x_ref[own, :].T
    wrote = pltpu.make_async_copy(basis_ref, basis_hbm, written.at[steps])
    wrote.start()
    y_ref[:128, :] = xb[own, :]
    y_ref[128:K, :] = xb[pl.ds(pl.multiple_of(128 - core * 128, 128), 128), :]
    parts = [v.astype(F32) for v in split3(jnp.broadcast_to(mean_ref[...], (16, D)))]
    line = lax.broadcasted_iota(jnp.int32, (16, D), 0)
    lines = jnp.where(line == 0, parts[0], jnp.where(line == 1, parts[1], parts[2]))
    lines = jnp.where(line < 3, lines, 0.0).astype(BF16)
    offset = jnp.sum(nt(lines, y_ref[:K, :]), axis=0, keepdims=True)
    mean_ref[:, :K] = offset

    def write(step):
        at = pl.ds(pl.multiple_of(step * STEP_ROWS, STEP_ROWS), STEP_ROWS)
        return pltpu.make_async_copy(out_ref.at[at], out_hbm.at[at], written.at[step])

    @pl.loop(0, steps)
    def _(step):
        fetch(step).wait()
        for r in range(0, STEP_ROWS, 256):
            at = pl.ds(pl.multiple_of(step * STEP_ROWS + r, 256), 256)
            coords = (nt(e_ref[at, :], y_ref[:K, :]) - mean_ref[:, :K]) * length_ref[at, :]
            squares = jnp.sum(coords * coords, axis=1, keepdims=True)
            scaled = coords[:, :128] * lax.rsqrt(squares * (1.0 / K) + 0.0001)
            out_ref[at, :] = scaled.astype(BF16)
        write(step).start()

    for step in range(steps):
        write(step).wait()
    wrote.wait()


def finished(embeddings, c_all, mu_all, b_all, length):
    rows = embeddings.shape[0]
    vm = pl.BlockSpec(memory_space=VMEM)
    hbm = pl.BlockSpec(memory_space=pltpu.HBM)
    return pl.pallas_call(
        finish_kernel,
        out_shape=(
            jax.ShapeDtypeStruct((rows, K // 2), BF16),
            jax.ShapeDtypeStruct((D, K // 2), F32),
        ),
        in_specs=[hbm] + [vm] * 4,
        out_specs=(hbm, hbm),
        scratch_shapes=[
            VMEM((rows, D), BF16),
            VMEM((K, D), F32),
            VMEM((1, D), F32),
            VMEM((K, D), BF16),
            VMEM((K, D), BF16),
            VMEM((K, 2 * K), F32),
            VMEM((2 * K, D), BF16),
            VMEM((rows, K // 2), BF16),
            VMEM((D, K // 2), F32),
            pltpu.SemaphoreType.DMA((rows // STEP_ROWS,)),
            pltpu.SemaphoreType.DMA((rows // STEP_ROWS + 1,)),
        ],
        compiler_params=pltpu.CompilerParams(vmem_limit_bytes=48 * 2**20),
        name="finish",
    )(embeddings, c_all, mu_all, b_all, length)


def shards(embeddings, start_basis):
    c_all, mu_all, b_all, length = gathered(embeddings, start_basis.T.astype(BF16))
    return tuple(finished(embeddings, c_all, mu_all, b_all, length))


def solution(mesh):
    in_specs = (P("rows", None), P(None, "cols"))
    out_specs = (P("rows", "cols"), P(None, "cols"))
    return jax.shard_map(shards, mesh=mesh, in_specs=in_specs, out_specs=out_specs, check_vma=False)
```

```python
import functools

import jax
import jax.numpy as jnp
from jax import lax
from jax.experimental import pallas as pl
from jax.experimental.pallas import tpu as pltpu
from jax.sharding import PartitionSpec as P

D = 1536
K = 256
B = 256
NB = D // B
OFFS = 4
MESH = pl.DeviceIdType.MESH
VMEM = pltpu.VMEM
F32 = jnp.float32
BF16 = jnp.bfloat16
STRIDES = (1, 4, 16)
STEP_ROWS = 512
LENGTH_ROWS = 256


def split3(v):
    high = v.astype(BF16)
    rest = v - high.astype(F32)
    mid = rest.astype(BF16)
    low = (rest - mid.astype(F32)).astype(BF16)
    return high, mid, low


def nt(a, b):
    return lax.dot_general(a, b, (((1,), (1,)), ((), ())), preferred_element_type=F32)


def nn(a, b):
    return lax.dot_general(a, b, (((1,), (0,)), ((), ())), preferred_element_type=F32)


def gather_kernel(
    rows, e_hbm, b_ref,
    c_out, apart_out, mean_out, b_out, length_out,
    e_ref, turned, s_ref, mu_ref, mu_out, sums, outer,
    got1, got2, got3, part2, fetched,
    send_rs, recv_rs, send_ag, recv_ag, send_cc, recv_cc, send_mu, recv_mu, send_x, recv_x,
):
    me = lax.axis_index("rows")
    core = lax.axis_index("cols")
    other = 1 - core
    coord = [lax.rem(me // s, 4) for s in STRIDES]
    steps = rows // STEP_ROWS

    def fetch(step):
        at = pl.ds(pl.multiple_of(step * STEP_ROWS, STEP_ROWS), STEP_ROWS)
        return pltpu.make_async_copy(e_hbm.at[at], e_ref.at[at], fetched.at[step])

    for step in range(steps):
        fetch(step).start()

    def peer(dim, o):
        return me + (lax.rem(coord[dim] + o, 4) - coord[dim]) * STRIDES[dim]

    barrier = pltpu.get_barrier_semaphore()
    for dim in range(3):
        for o in (1, 2, 3):
            pl.semaphore_signal(barrier, inc=1, device_id=(peer(dim, o), core), device_id_type=MESH)
    pl.semaphore_signal(barrier, inc=1, device_id=(me, other), device_id_type=MESH)

    sums[...] = jnp.zeros_like(sums)

    @pl.loop(0, steps)
    def _(step):
        fetch(step).wait()
        start = pl.multiple_of(step * STEP_ROWS, STEP_ROWS)
        for k in range(3):
            i = core * 3 + k
            part = e_ref[pl.ds(start, STEP_ROWS), pl.ds(pl.multiple_of(i * B, B), B)]
            turned[k * B : k * B + B, pl.ds(start, STEP_ROWS)] = part.T
        for q in range(NB):
            at = slice(q * B, q * B + B)
            total = sums[:, at]
            for r in range(0, STEP_ROWS, 16):
                total = total + e_ref[pl.ds(start + r, 16), at].astype(F32)
            sums[:, at] = total

    whole = jnp.sum(sums[...], axis=0, keepdims=True)
    mean = whole * (1.0 / rows)
    sums[0:1, :] = mean
    for k in range(3):
        for half in range(2):
            at = pl.ds(pl.multiple_of((core * 3 + k) * B + half * 128, 128), 128)
            mu_ref[2 * k + half : 2 * k + half + 1, :] = sums[0:1, at]
    mu_ref[6:8, :] = jnp.zeros((2, 128), F32)
    place = coord[0] * 16 + coord[1] * 4 + coord[2]
    mu_out[core, place] = mu_ref[...]
    b_out[core] = b_ref[...]

    started = []

    def send(src, dst, send_sem, recv_sem, to):
        copy = pltpu.make_async_remote_copy(
            src_ref=src, dst_ref=dst, send_sem=send_sem, recv_sem=recv_sem,
            device_id=to, device_id_type=MESH,
        )
        copy.start()
        started.append(copy)
        return copy

    def rows_of(k, start, size):
        return pl.ds(pl.multiple_of(k * 1024 + start, 16), size)

    pl.semaphore_wait(barrier, 10)

    def send_means(n, at):
        return [
            send(
                mu_out.at[core, at], mu_out.at[core, at],
                send_mu.at[n, o - 1], recv_mu.at[n, o - 1], (peer(2 - n, o), core),
            )
            for o in (2, 1, 3)
        ]

    means = send_means(0, pl.ds(place, 1))
    b_copy = send(b_ref, b_out.at[core], send_x.at[0], recv_x.at[0], (me, other))

    line = lax.broadcasted_iota(jnp.int32, (16, D), 0)

    def lines(v, order):
        parts = split3(jnp.broadcast_to(v, (16, D)))
        out = jnp.zeros((16, D), F32)
        for n, which in enumerate(order):
            out = jnp.where(line == n, parts[which].astype(F32), out)
        return out.astype(BF16)

    outer[:16, :] = lines(whole, (0, 0, 1, 1, 0, 2))
    outer[16:, :] = lines(-mean, (0, 1, 0, 1, 2, 0))

    def first_copy(k, o):
        block = rows_of(k, lax.rem(coord[k] + o, 4) * 256, 256)
        return pltpu.make_async_remote_copy(
            src_ref=s_ref.at[block], dst_ref=got1.at[k, o - 1],
            send_sem=send_rs.at[0, k, o - 1], recv_sem=recv_rs.at[0, k, o - 1],
            device_id=(peer(k, o), core), device_id_type=MESH,
        )

    for k in range(3):
        i = core * 3 + k
        left = outer[:16, pl.ds(pl.multiple_of(i * B, B), B)]

        @pl.loop(0, OFFS)
        def _(n):
            o = OFFS - 1 - n
            to = lax.rem(coord[k] + o, 4)
            at = pl.ds(pl.multiple_of(lax.rem(i + to, NB) * B, B), B)
            total = nn(turned[k * B : k * B + B, :], e_ref[:, at])
            total = total + lax.dot_general(
                left, outer[16:, at], (((0,), (0,)), ((), ())), preferred_element_type=F32
            )
            s_ref[rows_of(k, to * 256, 256), :] = total.astype(BF16)

            @pl.when(o > 0)
            def _():
                first_copy(k, o).start()

        if k == 0:
            for copy in means:
                copy.wait_recv()
            means = send_means(1, pl.ds(pl.multiple_of(place // 4 * 4, 4), 4))
    for copy in means:
        copy.wait_recv()
    means = send_means(2, pl.ds(pl.multiple_of(coord[0] * 16, 16), 16))

    second = {}
    for k in range(3):
        for o in (1, 2, 3):
            first_copy(k, o).wait_recv()
        total = s_ref[rows_of(k, coord[k] * 256, 256), :].astype(F32)
        for o in range(3):
            total = total + got1[k, o].astype(F32)
        part2[k] = total.astype(BF16)
        d = (k + 1) % 3
        for o in (2, 1, 3):
            to = lax.rem(coord[d] + o, 4)
            second[k, o] = send(
                part2.at[k, pl.ds(pl.multiple_of(to * 64, 16), 64)], got2.at[k, o - 1],
                send_rs.at[1, k, o - 1], recv_rs.at[1, k, o - 1], (peer(d, o), core),
            )

    for copy in means:
        copy.wait_recv()
    mu_copy = send(mu_out.at[core], mu_out.at[core], send_x.at[1], recv_x.at[1], (me, other))

    third = {}
    for k in range(3):
        d = (k + 1) % 3
        for o in (1, 2, 3):
            second[k, o].wait_recv()
        total = part2[k, pl.ds(pl.multiple_of(coord[d] * 64, 16), 64), :].astype(F32)
        for o in range(3):
            total = total + got2[k, o].astype(F32)
        d = (k + 2) % 3
        got3[k, coord[d]] = total.astype(BF16)
        for o in (2, 1, 3):
            third[k, o] = send(
                got3.at[k, coord[d]], got3.at[k, coord[d]],
                send_rs.at[2, k, o - 1], recv_rs.at[2, k, o - 1], (peer(d, o), core),
            )
    spread = {}
    for k in range(3):
        a, b = (coord[(k + n) % 3] for n in range(2))
        d = (k + 1) % 3
        for o in (1, 2, 3):
            third[k, o].wait_recv()
        total = got3[k, 0].astype(F32)
        for c in range(1, 4):
            total = total + got3[k, c].astype(F32)
        mine = rows_of(k, (a * 4 + b) * 64, 64)
        c_out[core, mine, :] = total.astype(BF16)
        for o in (2, 1, 3):
            spread[1, k, o] = send(
                c_out.at[core, mine], c_out.at[core, mine],
                send_ag.at[0, k, o - 1], recv_ag.at[0, k, o - 1], (peer(d, o), core),
            )
    across = []
    for k in range(3):
        a = coord[k]
        for o in (1, 2, 3):
            spread[1, k, o].wait_recv()
        mine = rows_of(k, a * 256, 256)
        for o in (2, 1, 3):
            spread[2, k, o] = send(
                c_out.at[core, mine], c_out.at[core, mine],
                send_ag.at[1, k, o - 1], recv_ag.at[1, k, o - 1], (peer(k, o), core),
            )
        across.append(
            send(
                c_out.at[core, mine], c_out.at[core, mine],
                send_cc.at[k, 0], recv_cc.at[k, 0], (me, other),
            )
        )
    mu_copy.wait_recv()
    for h in range(2):
        for q in range(6):
            at = slice((h * 6 + q) * 128, (h * 6 + q + 1) * 128)
            part = mu_out[h, :, q, :]
            center = jnp.mean(part, axis=0, keepdims=True)
            mean_out[:, at] = center
            part = part - center
            high = part.astype(BF16)
            low = (part - high.astype(F32)).astype(BF16)
            apart_out[:, at] = jnp.concatenate([high, low, high, low], axis=0)

    @pl.loop(0, rows // LENGTH_ROWS)
    def _(n):
        at = pl.ds(pl.multiple_of(n * LENGTH_ROWS, LENGTH_ROWS), LENGTH_ROWS)
        apart = e_ref[at, :].astype(F32) - mean_out[...]
        length_out[at, :] = lax.rsqrt(jnp.sum(apart * apart, axis=1, keepdims=True) + 1.0)

    for o in (1, 3, 2):
        for k in range(3):
            spread[2, k, o].wait_recv()
            got = rows_of(k, lax.rem(coord[k] + 4 - o, 4) * 256, 256)
            across.append(
                send(
                    c_out.at[core, got], c_out.at[core, got],
                    send_cc.at[k, o], recv_cc.at[k, o], (me, other),
                )
            )
    for copy in across:
        copy.wait_recv()
    b_copy.wait_recv()
    for copy in started:
        copy.wait_send()
    for k in range(3):
        for o in (1, 2, 3):
            first_copy(k, o).wait_send()


def gathered(embeddings, b):
    rows = embeddings.shape[0]
    size = 3 * OFFS * B
    sem = pltpu.SemaphoreType.DMA
    vm = pl.BlockSpec(memory_space=VMEM)
    return pl.pallas_call(
        functools.partial(gather_kernel, rows),
        out_shape=(
            jax.ShapeDtypeStruct((2, size, B), BF16),
            jax.ShapeDtypeStruct((K, D), BF16),
            jax.ShapeDtypeStruct((1, D), F32),
            jax.ShapeDtypeStruct((2, *b.shape), BF16),
            jax.ShapeDtypeStruct((rows, 1), F32),
        ),
        in_specs=[pl.BlockSpec(memory_space=pltpu.HBM), vm],
        out_specs=(vm,) * 5,
        scratch_shapes=[
            VMEM((rows, D), BF16),
            VMEM((3 * B, rows), BF16),
            VMEM((size, B), BF16),
            VMEM((8, 128), F32),
            VMEM((2, 64, 8, 128), F32),
            VMEM((16, D), F32),
            VMEM((32, D), BF16),
            VMEM((3, 3, 256, B), BF16),
            VMEM((3, 3, 64, B), BF16),
            VMEM((3, 4, 64, B), BF16),
            VMEM((3, 256, B), BF16),
            sem((rows // STEP_ROWS,)),
            sem((3, 3, 3)), sem((3, 3, 3)),
            sem((2, 3, 3)), sem((2, 3, 3)),
            sem((3, 4)), sem((3, 4)),
            sem((3, 3)), sem((3, 3)),
            sem((2,)), sem((2,)),
        ],
        compiler_params=pltpu.CompilerParams(
            collective_id=0, has_side_effects=True, vmem_limit_bytes=46 * 2**20
        ),
        name="gather",
    )(embeddings, b)


PANEL = 32
ROWS_ALL = 196608.0


def factor_panel(a_ref, at):
    low, high = (0, 3) if at < 128 else (1, 4)
    tiles = range(low, high)
    home = at // 128
    groups = PANEL // 8
    rows = [
        [a_ref[at + 8 * g : at + 8 * g + 8, 128 * t : 128 * t + 128] for t in tiles]
        for g in range(groups)
    ]
    line = lax.broadcasted_iota(jnp.int32, (8, 128), 0)
    done = []
    for g in range(groups):
        first = at + 8 * g - 128 * home
        cols = [
            [
                jnp.broadcast_to(rows[t][home - low][:, first + c : first + c + 1], (8, 128))
                for c in range(8)
            ]
            for t in range(g, groups)
        ]
        scale = None
        pivot = jnp.broadcast_to(cols[0][0][0:1, :], (8, 128))
        for j in range(8):
            root = lax.rsqrt(pivot)
            scale = root if scale is None else jnp.where(line >= j, root, scale)
            inverse = root * root
            heads = [
                jnp.broadcast_to(cols[0][c][j : j + 1, :], (8, 128)) for c in range(j + 1, 8)
            ]
            if j < 7:
                pivot = jnp.broadcast_to(cols[0][j + 1][j + 1 : j + 2, :], (8, 128))
                pivot = pivot - heads[0] * heads[0] * inverse
            source = [jnp.broadcast_to(v[j : j + 1, :], (8, 128)) for v in rows[g]]
            for t in range(g, groups):
                m = cols[t - g][j]
                if t == g:
                    m = jnp.where(line > j, m, 0.0)
                m = m * inverse
                for c in range(j + 1, 8):
                    cols[t - g][c] = cols[t - g][c] - m * heads[c - j - 1]
                rows[t] = [v - m * s for v, s in zip(rows[t], source)]
        rows[g] = [v * scale for v in rows[g]]
        done.append(rows[g])
    for g in range(groups):
        for t, v in zip(tiles, done[g]):
            a_ref[at + 8 * g : at + 8 * g + 8, 128 * t : 128 * t + 128] = v
    left = K - at - PANEL
    if left:
        whole = [jnp.concatenate([done[g][n] for g in range(groups)], axis=0) for n in range(3)]
        whole = jnp.concatenate(whole, axis=1)
        high_, mid, low_ = split3(whole)
        right = jnp.concatenate([high_, mid, high_, low_, high_, mid], axis=0)
        side = jnp.concatenate([high_, high_, mid, high_, low_, mid], axis=0)
        side = side[:, : (2 - low) * 128]
        change = lax.dot_general(
            side, right, (((0,), (0,)), ((), ())), preferred_element_type=F32
        )
        skip = at + PANEL - 128 * low
        cols = slice(128 * low, 128 * high)
        a_ref[at + PANEL : K, cols] = a_ref[at + PANEL : K, cols] - change[skip:, :]


def finish_kernel(
    e_hbm, c_ref, apart, mean_ref, b_ref, length_ref, out_hbm, basis_hbm,
    e_ref, x_ref, offset, xb, a_ref, y_ref, out_ref, basis_ref, fetched, written,
):
    rows = e_ref.shape[0]
    steps = rows // STEP_ROWS

    def fetch(step):
        at = pl.ds(pl.multiple_of(step * STEP_ROWS, STEP_ROWS), STEP_ROWS)
        return pltpu.make_async_copy(e_hbm.at[at], e_ref.at[at], fetched.at[step])

    for step in range(steps):
        fetch(step).start()
    for h in range(2):
        xb[128 * h : 128 * h + 128, :] = b_ref[h]

    @pl.loop(0, 3)
    def _(step):
        t = nt(xb[...], apart[:128, :]) * float(rows)
        t = t + pltpu.roll(t, 64, 1)
        high = t.astype(BF16)
        low = (t - high.astype(F32)).astype(BF16)
        t = jnp.concatenate([high, low], axis=1)
        for j in range(NB):
            at = slice(j * B, j * B + B)
            total = nn(t, apart[:, at])
            for i in range(NB):
                o = (j - i) % NB
                left = xb[:, i * B : i * B + B]
                if o < OFFS:
                    r = (i % 3 * OFFS + o) * B
                    total = total + nn(left, c_ref[i // 3, r : r + B, :])
                else:
                    r = (j % 3 * OFFS + NB - o) * B
                    total = total + nt(left, c_ref[j // 3, r : r + B, :])
            total = total * (1.0 / ROWS_ALL)
            high = total.astype(BF16)
            y_ref[:K, at] = high
            y_ref[K:, at] = (total - high.astype(F32)).astype(BF16)

        @pl.when(step == 0)
        def _():
            xb[...] = y_ref[:K, :]

        @pl.when(step > 0)
        def _():
            g = nt(y_ref[...], y_ref[...])
            g = g[:K, :K] + g[K:, K:] + (g[:K, K:] + g[K:, :K])
            a_ref[:, :K] = g
            a_ref[:, K:] = (
                lax.broadcasted_iota(jnp.int32, (K, K), 0)
                == lax.broadcasted_iota(jnp.int32, (K, K), 1)
            ).astype(F32)
            for at in range(0, K // 2, PANEL):
                factor_panel(a_ref, at)

            @pl.when(step == 1)
            def _():
                low = a_ref[K // 2 :, K // 2 : K]
                diagonal = lax.broadcasted_iota(jnp.int32, low.shape, 0) == (
                    lax.broadcasted_iota(jnp.int32, low.shape, 1)
                )
                size = jnp.sum(jnp.where(diagonal, low, 0.0), axis=1, keepdims=True)
                a_ref[K // 2 :, K:] = a_ref[K // 2 :, K:] * lax.rsqrt(size)

            @pl.when(step == 2)
            def _():
                for at in range(K // 2, K, PANEL):
                    factor_panel(a_ref, at)

            inverse = a_ref[:, K:]
            inverse = jnp.where(
                lax.broadcasted_iota(jnp.int32, (K, K), 0)
                >= lax.broadcasted_iota(jnp.int32, (K, K), 1),
                inverse, 0.0,
            )
            high = inverse.astype(BF16)
            low = (inverse - high.astype(F32)).astype(BF16)
            for j in range(NB):
                at = slice(j * B, j * B + B)
                x = nn(high, y_ref[:K, at]) + (nn(low, y_ref[:K, at]) + nn(high, y_ref[K:, at]))
                x_ref[:, at] = x
                xb[:, at] = x.astype(BF16)

    core = lax.axis_index("cols")
    own = pl.ds(pl.multiple_of(core * 128, 128), 128)
    basis_ref[...] = x_ref[own, :].T
    wrote = pltpu.make_async_copy(basis_ref, basis_hbm, written.at[steps])
    wrote.start()
    y_ref[:128, :] = xb[own, :]
    y_ref[128:K, :] = xb[pl.ds(pl.multiple_of(128 - core * 128, 128), 128), :]
    parts = [v.astype(F32) for v in split3(jnp.broadcast_to(mean_ref[...], (16, D)))]
    line = lax.broadcasted_iota(jnp.int32, (16, D), 0)
    lines = jnp.where(line == 0, parts[0], jnp.where(line == 1, parts[1], parts[2]))
    lines = jnp.where(line < 3, lines, 0.0).astype(BF16)
    offset[...] = jnp.sum(nt(lines, y_ref[:K, :]), axis=0, keepdims=True)

    def write(step):
        at = pl.ds(pl.multiple_of(step * STEP_ROWS, STEP_ROWS), STEP_ROWS)
        return pltpu.make_async_copy(out_ref.at[at], out_hbm.at[at], written.at[step])

    @pl.loop(0, steps)
    def _(step):
        fetch(step).wait()
        for r in range(0, STEP_ROWS, 256):
            at = pl.ds(pl.multiple_of(step * STEP_ROWS + r, 256), 256)
            coords = (nt(e_ref[at, :], y_ref[:K, :]) - offset[...]) * length_ref[at, :]
            squares = jnp.sum(coords * coords, axis=1, keepdims=True)
            scaled = coords[:, :128] * lax.rsqrt(squares * (1.0 / K) + 0.0001)
            out_ref[at, :] = scaled.astype(BF16)
        write(step).start()

    for step in range(steps):
        write(step).wait()
    wrote.wait()


def finished(embeddings, c_all, apart, mean, b_all, length):
    rows = embeddings.shape[0]
    vm = pl.BlockSpec(memory_space=VMEM)
    hbm = pl.BlockSpec(memory_space=pltpu.HBM)
    return pl.pallas_call(
        finish_kernel,
        out_shape=(
            jax.ShapeDtypeStruct((rows, K // 2), BF16),
            jax.ShapeDtypeStruct((D, K // 2), F32),
        ),
        in_specs=[hbm] + [vm] * 5,
        out_specs=(hbm, hbm),
        scratch_shapes=[
            VMEM((rows, D), BF16),
            VMEM((K, D), F32),
            VMEM((1, K), F32),
            VMEM((K, D), BF16),
            VMEM((K, 2 * K), F32),
            VMEM((2 * K, D), BF16),
            VMEM((rows, K // 2), BF16),
            VMEM((D, K // 2), F32),
            pltpu.SemaphoreType.DMA((rows // STEP_ROWS,)),
            pltpu.SemaphoreType.DMA((rows // STEP_ROWS + 1,)),
        ],
        compiler_params=pltpu.CompilerParams(vmem_limit_bytes=47 * 2**20),
        name="finish",
    )(embeddings, c_all, apart, mean, b_all, length)


def shards(embeddings, start_basis):
    parts = gathered(embeddings, start_basis.T.astype(BF16))
    return tuple(finished(embeddings, *parts))


def solution(mesh):
    in_specs = (P("rows", None), P(None, "cols"))
    out_specs = (P("rows", "cols"), P(None, "cols"))
    return jax.shard_map(shards, mesh=mesh, in_specs=in_specs, out_specs=out_specs, check_vma=False)
```

```python
import functools

import jax
import jax.numpy as jnp
from jax import lax
from jax.experimental import pallas as pl
from jax.experimental.pallas import tpu as pltpu
from jax.sharding import PartitionSpec as P

D = 1536
K = 256
B = 256
NB = D // B
OFFS = 4
MESH = pl.DeviceIdType.MESH
VMEM = pltpu.VMEM
F32 = jnp.float32
BF16 = jnp.bfloat16
STRIDES = (1, 4, 16)
STEP_ROWS = 512
LENGTH_ROWS = 256


def split3(v):
    high = v.astype(BF16)
    rest = v - high.astype(F32)
    mid = rest.astype(BF16)
    low = (rest - mid.astype(F32)).astype(BF16)
    return high, mid, low


def nt(a, b):
    return lax.dot_general(a, b, (((1,), (1,)), ((), ())), preferred_element_type=F32)


def nn(a, b):
    return lax.dot_general(a, b, (((1,), (0,)), ((), ())), preferred_element_type=F32)


def gather_kernel(
    rows, e_hbm, start_hbm,
    c_out, apart_out, mean_out, b_out, length_out,
    e_ref, turned, s_ref, mu_ref, mu_out, start_ref, sums,
    got1, got2, got3, part2, fetched,
    send_rs, recv_rs, send_ag, recv_ag, send_cc, recv_cc, send_mu, recv_mu, send_x, recv_x,
):
    me = lax.axis_index("rows")
    core = lax.axis_index("cols")
    other = 1 - core
    coord = [lax.rem(me // s, 4) for s in STRIDES]
    steps = rows // STEP_ROWS

    def fetch(step):
        at = pl.ds(pl.multiple_of(step * STEP_ROWS, STEP_ROWS), STEP_ROWS)
        return pltpu.make_async_copy(e_hbm.at[at], e_ref.at[at], fetched.at[step])

    for step in range(steps):
        fetch(step).start()
    start_copy = pltpu.make_async_copy(start_hbm, start_ref, fetched.at[steps])
    start_copy.start()

    def peer(dim, o):
        return me + (lax.rem(coord[dim] + o, 4) - coord[dim]) * STRIDES[dim]

    barrier = pltpu.get_barrier_semaphore()
    for dim in range(3):
        for o in (1, 2, 3):
            pl.semaphore_signal(barrier, inc=1, device_id=(peer(dim, o), core), device_id_type=MESH)
    pl.semaphore_signal(barrier, inc=1, device_id=(me, other), device_id_type=MESH)

    sums[...] = jnp.zeros_like(sums)

    @pl.loop(0, steps)
    def _(step):
        fetch(step).wait()
        start = pl.multiple_of(step * STEP_ROWS, STEP_ROWS)
        for k in range(3):
            i = core * 3 + k
            part = e_ref[pl.ds(start, STEP_ROWS), pl.ds(pl.multiple_of(i * B, B), B)]
            turned[k * B : k * B + B, pl.ds(start, STEP_ROWS)] = part.T
        for q in range(NB):
            at = slice(q * B, q * B + B)
            total = sums[:, at]
            for r in range(0, STEP_ROWS, 16):
                total = total + e_ref[pl.ds(start + r, 16), at].astype(F32)
            sums[:, at] = total

    whole = jnp.sum(sums[...], axis=0, keepdims=True)
    mean = whole * (1.0 / rows)
    sums[0:1, :] = mean
    for k in range(3):
        for half in range(2):
            at = pl.ds(pl.multiple_of((core * 3 + k) * B + half * 128, 128), 128)
            mu_ref[2 * k + half : 2 * k + half + 1, :] = sums[0:1, at]
    mu_ref[6:8, :] = jnp.zeros((2, 128), F32)
    place = coord[0] * 16 + coord[1] * 4 + coord[2]
    mu_out[core, place] = mu_ref[...]

    started = []

    def send(src, dst, send_sem, recv_sem, to):
        copy = pltpu.make_async_remote_copy(
            src_ref=src, dst_ref=dst, send_sem=send_sem, recv_sem=recv_sem,
            device_id=to, device_id_type=MESH,
        )
        copy.start()
        started.append(copy)
        return copy

    def rows_of(k, start, size):
        return pl.ds(pl.multiple_of(k * 1024 + start, 16), size)

    pl.semaphore_wait(barrier, 10)

    def send_means(n, at):
        return [
            send(
                mu_out.at[core, at], mu_out.at[core, at],
                send_mu.at[n, o - 1], recv_mu.at[n, o - 1], (peer(2 - n, o), core),
            )
            for o in (2, 1, 3)
        ]

    means = send_means(0, pl.ds(place, 1))

    line = lax.broadcasted_iota(jnp.int32, (16, D), 0)

    def lines(v, order):
        parts = split3(jnp.broadcast_to(v, (16, D)))
        out = jnp.zeros((16, D), F32)
        for n, which in enumerate(order):
            out = jnp.where(line == n, parts[which].astype(F32), out)
        return out.astype(BF16)

    e_ref[rows:, :] = lines(-mean, (0, 1, 0, 1, 2, 0))
    s_ref[:16 * NB, :] = jnp.concatenate(
        [lines(whole, (0, 0, 1, 1, 0, 2))[:, q * B : q * B + B] for q in range(NB)], axis=0
    )
    for k in range(3):
        part = s_ref[pl.ds(pl.multiple_of((core * 3 + k) * 16, 16), 16), :]
        part = jnp.concatenate([part, jnp.zeros((112, B), BF16)], axis=0)
        turned[k * B : k * B + B, rows:] = part.T

    def first_copy(k, o):
        block = rows_of(k, lax.rem(coord[k] + o, 4) * 256, 256)
        return pltpu.make_async_remote_copy(
            src_ref=s_ref.at[block], dst_ref=got1.at[k, o - 1],
            send_sem=send_rs.at[0, k, o - 1], recv_sem=recv_rs.at[0, k, o - 1],
            device_id=(peer(k, o), core), device_id_type=MESH,
        )

    for k in range(3):
        i = core * 3 + k

        @pl.loop(0, OFFS)
        def _(n):
            o = OFFS - 1 - n
            to = lax.rem(coord[k] + o, 4)
            at = pl.ds(pl.multiple_of(lax.rem(i + to, NB) * B, B), B)
            total = nn(turned[k * B : k * B + B, : rows + 16], e_ref[:, at])
            s_ref[rows_of(k, to * 256, 256), :] = total.astype(BF16)

            @pl.when(o > 0)
            def _():
                first_copy(k, o).start()

        if k == 0:
            for copy in means:
                copy.wait_recv()
            means = send_means(1, pl.ds(pl.multiple_of(place // 4 * 4, 4), 4))
    for copy in means:
        copy.wait_recv()
    means = send_means(2, pl.ds(pl.multiple_of(coord[0] * 16, 16), 16))
    start_copy.wait()
    b_out[core] = start_ref[...].T.astype(BF16)
    b_copy = send(b_out.at[core], b_out.at[core], send_x.at[0], recv_x.at[0], (me, other))

    second = {}
    for k in range(3):
        for o in (1, 2, 3):
            first_copy(k, o).wait_recv()
        total = s_ref[rows_of(k, coord[k] * 256, 256), :].astype(F32)
        for o in range(3):
            total = total + got1[k, o].astype(F32)
        part2[k] = total.astype(BF16)
        d = (k + 1) % 3
        for o in (2, 1, 3):
            to = lax.rem(coord[d] + o, 4)
            second[k, o] = send(
                part2.at[k, pl.ds(pl.multiple_of(to * 64, 16), 64)], got2.at[k, o - 1],
                send_rs.at[1, k, o - 1], recv_rs.at[1, k, o - 1], (peer(d, o), core),
            )

    for copy in means:
        copy.wait_recv()
    mu_copy = send(mu_out.at[core], mu_out.at[core], send_x.at[1], recv_x.at[1], (me, other))

    third = {}
    for k in range(3):
        d = (k + 1) % 3
        for o in (1, 2, 3):
            second[k, o].wait_recv()
        total = part2[k, pl.ds(pl.multiple_of(coord[d] * 64, 16), 64), :].astype(F32)
        for o in range(3):
            total = total + got2[k, o].astype(F32)
        d = (k + 2) % 3
        got3[k, coord[d]] = total.astype(BF16)
        for o in (2, 1, 3):
            third[k, o] = send(
                got3.at[k, coord[d]], got3.at[k, coord[d]],
                send_rs.at[2, k, o - 1], recv_rs.at[2, k, o - 1], (peer(d, o), core),
            )
    spread = {}
    for k in range(3):
        a, b = (coord[(k + n) % 3] for n in range(2))
        d = (k + 1) % 3
        for o in (1, 2, 3):
            third[k, o].wait_recv()
        total = got3[k, 0].astype(F32)
        for c in range(1, 4):
            total = total + got3[k, c].astype(F32)
        mine = rows_of(k, (a * 4 + b) * 64, 64)
        c_out[core, mine, :] = total.astype(BF16)
        for o in (2, 1, 3):
            spread[1, k, o] = send(
                c_out.at[core, mine], c_out.at[core, mine],
                send_ag.at[0, k, o - 1], recv_ag.at[0, k, o - 1], (peer(d, o), core),
            )
    across = []
    for k in range(3):
        a = coord[k]
        for o in (1, 2, 3):
            spread[1, k, o].wait_recv()
        mine = rows_of(k, a * 256, 256)
        for o in (2, 1, 3):
            spread[2, k, o] = send(
                c_out.at[core, mine], c_out.at[core, mine],
                send_ag.at[1, k, o - 1], recv_ag.at[1, k, o - 1], (peer(k, o), core),
            )
        across.append(
            send(
                c_out.at[core, mine], c_out.at[core, mine],
                send_cc.at[k, 0], recv_cc.at[k, 0], (me, other),
            )
        )
    mu_copy.wait_recv()
    for h in range(2):
        for q in range(6):
            at = slice((h * 6 + q) * 128, (h * 6 + q + 1) * 128)
            part = mu_out[h, :, q, :]
            center = jnp.mean(part, axis=0, keepdims=True)
            mean_out[:, at] = center
            part = part - center
            high = part.astype(BF16)
            low = (part - high.astype(F32)).astype(BF16)
            apart_out[:, at] = jnp.concatenate([high, low, high, low], axis=0)

    @pl.loop(0, rows // LENGTH_ROWS)
    def _(n):
        at = pl.ds(pl.multiple_of(n * LENGTH_ROWS, LENGTH_ROWS), LENGTH_ROWS)
        apart = e_ref[at, :].astype(F32) - mean_out[...]
        length_out[at, :] = lax.rsqrt(jnp.sum(apart * apart, axis=1, keepdims=True) + 1.0)

    for o in (1, 3, 2):
        for k in range(3):
            spread[2, k, o].wait_recv()
            got = rows_of(k, lax.rem(coord[k] + 4 - o, 4) * 256, 256)
            across.append(
                send(
                    c_out.at[core, got], c_out.at[core, got],
                    send_cc.at[k, o], recv_cc.at[k, o], (me, other),
                )
            )
    for copy in across:
        copy.wait_recv()
    b_copy.wait_recv()
    for copy in started:
        copy.wait_send()
    for k in range(3):
        for o in (1, 2, 3):
            first_copy(k, o).wait_send()


def gathered(embeddings, start_basis):
    rows = embeddings.shape[0]
    size = 3 * OFFS * B
    sem = pltpu.SemaphoreType.DMA
    vm = pl.BlockSpec(memory_space=VMEM)
    return pl.pallas_call(
        functools.partial(gather_kernel, rows),
        out_shape=(
            jax.ShapeDtypeStruct((2, size, B), BF16),
            jax.ShapeDtypeStruct((K, D), BF16),
            jax.ShapeDtypeStruct((1, D), F32),
            jax.ShapeDtypeStruct((2, K // 2, D), BF16),
            jax.ShapeDtypeStruct((rows, 1), F32),
        ),
        in_specs=[pl.BlockSpec(memory_space=pltpu.HBM)] * 2,
        out_specs=(vm,) * 5,
        scratch_shapes=[
            VMEM((rows + 16, D), BF16),
            VMEM((3 * B, rows + 128), BF16),
            VMEM((size, B), BF16),
            VMEM((8, 128), F32),
            VMEM((2, 64, 8, 128), F32),
            VMEM((D, K // 2), F32),
            VMEM((16, D), F32),
            VMEM((3, 3, 256, B), BF16),
            VMEM((3, 3, 64, B), BF16),
            VMEM((3, 4, 64, B), BF16),
            VMEM((3, 256, B), BF16),
            sem((rows // STEP_ROWS + 1,)),
            sem((3, 3, 3)), sem((3, 3, 3)),
            sem((2, 3, 3)), sem((2, 3, 3)),
            sem((3, 4)), sem((3, 4)),
            sem((3, 3)), sem((3, 3)),
            sem((2,)), sem((2,)),
        ],
        compiler_params=pltpu.CompilerParams(
            collective_id=0, has_side_effects=True, vmem_limit_bytes=46 * 2**20
        ),
        name="gather",
    )(embeddings, start_basis)


PANEL = 32
WIDE = 16
ROWS_ALL = 196608.0


def factor_panel(a_ref, at):
    low, high = (0, 3) if at < 128 else (1, 4)
    tiles = range(low, high)
    home = at // 128
    groups = PANEL // 8
    rows = [
        [a_ref[at + 8 * g : at + 8 * g + 8, 128 * t : 128 * t + 128] for t in tiles]
        for g in range(groups)
    ]
    line = lax.broadcasted_iota(jnp.int32, (8, 128), 0)
    def spread(v, sublane):
        return jnp.broadcast_to(v[sublane : sublane + 1, :], (8, 128))

    done = []
    for base in range(0, groups, WIDE // 8):
        first = at + 8 * base - 128 * home
        cols = [
            {
                t: jnp.broadcast_to(
                    rows[t][home - low][:, first + c : first + c + 1], (8, 128)
                )
                for t in range(base + c // 8, groups)
            }
            for c in range(WIDE)
        ]
        pivot = spread(cols[0][base], 0)
        for c in range(WIDE):
            g, j = base + c // 8, c % 8
            root = lax.rsqrt(pivot)
            scale = root if j == 0 else jnp.where(line >= j, root, scale)
            inverse = root * root
            heads = {n: spread(cols[c][base + n // 8], n % 8) for n in range(c + 1, WIDE)}
            if c + 1 < WIDE:
                pivot = spread(cols[c + 1][base + (c + 1) // 8], (c + 1) % 8)
                pivot = pivot - heads[c + 1] * heads[c + 1] * inverse
            source = [spread(v, j) for v in rows[g]]
            for t in range(g, groups):
                m = cols[c][t]
                if t == g:
                    m = jnp.where(line > j, m, 0.0)
                m = m * inverse
                for n in range(c + 1, WIDE):
                    if t >= base + n // 8:
                        cols[n][t] = cols[n][t] - m * heads[n]
                rows[t] = [v - m * s for v, s in zip(rows[t], source)]
            if j == 7:
                rows[g] = [v * scale for v in rows[g]]
                done.append(rows[g])
    for g in range(groups):
        for t, v in zip(tiles, done[g]):
            a_ref[at + 8 * g : at + 8 * g + 8, 128 * t : 128 * t + 128] = v
    left = K - at - PANEL
    if left:
        whole = [jnp.concatenate([done[g][n] for g in range(groups)], axis=0) for n in range(3)]
        whole = jnp.concatenate(whole, axis=1)
        high_, mid, low_ = split3(whole)
        right = jnp.concatenate([high_, mid, high_, low_, high_, mid], axis=0)
        side = jnp.concatenate([high_, high_, mid, high_, low_, mid], axis=0)
        side = side[:, : (2 - low) * 128]
        change = lax.dot_general(
            side, right, (((0,), (0,)), ((), ())), preferred_element_type=F32
        )
        skip = at + PANEL - 128 * low
        cols = slice(128 * low, 128 * high)
        a_ref[at + PANEL : K, cols] = a_ref[at + PANEL : K, cols] - change[skip:, :]


def finish_kernel(
    e_hbm, c_ref, apart, mean_ref, b_ref, length_ref, out_hbm, basis_hbm,
    e_ref, x_ref, offset, xb, a_ref, y_ref, out_ref, basis_ref, fetched, written,
):
    rows = e_ref.shape[0]
    steps = rows // STEP_ROWS

    def fetch(step):
        at = pl.ds(pl.multiple_of(step * STEP_ROWS, STEP_ROWS), STEP_ROWS)
        return pltpu.make_async_copy(e_hbm.at[at], e_ref.at[at], fetched.at[step])

    for step in range(steps):
        fetch(step).start()
    for h in range(2):
        xb[128 * h : 128 * h + 128, :] = b_ref[h]

    @pl.loop(0, 3)
    def _(step):
        t = nt(xb[...], apart[:128, :]) * float(rows)
        t = t + pltpu.roll(t, 64, 1)
        high = t.astype(BF16)
        low = (t - high.astype(F32)).astype(BF16)
        t = jnp.concatenate([high, low], axis=1)
        for j in range(NB):
            at = slice(j * B, j * B + B)
            total = nn(t, apart[:, at])
            for i in range(NB):
                o = (j - i) % NB
                left = xb[:, i * B : i * B + B]
                if o < OFFS:
                    r = (i % 3 * OFFS + o) * B
                    total = total + nn(left, c_ref[i // 3, r : r + B, :])
                else:
                    r = (j % 3 * OFFS + NB - o) * B
                    total = total + nt(left, c_ref[j // 3, r : r + B, :])
            total = total * (1.0 / ROWS_ALL)
            high = total.astype(BF16)
            y_ref[:K, at] = high
            y_ref[K:, at] = (total - high.astype(F32)).astype(BF16)

        @pl.when(step == 0)
        def _():
            xb[...] = y_ref[:K, :]

        @pl.when(step > 0)
        def _():
            def gram(half):
                at = slice(half * 128, half * 128 + 128)
                high = nt(y_ref[at, :], y_ref[...])
                low = nt(y_ref[K + half * 128 : K + half * 128 + 128, :], y_ref[...])
                a_ref[at, :K] = high[:, :K] + low[:, K:] + (high[:, K:] + low[:, :K])

            gram(0)

            @pl.when(step == 1)
            def _():
                a_ref[K // 2 :, :K] = jnp.zeros((K // 2, K), F32)

            @pl.when(step == 2)
            def _():
                gram(1)

            a_ref[:, K:] = (
                lax.broadcasted_iota(jnp.int32, (K, K), 0)
                == lax.broadcasted_iota(jnp.int32, (K, K), 1)
            ).astype(F32)
            for at in range(0, K // 2, PANEL):
                factor_panel(a_ref, at)

            @pl.when(step == 1)
            def _():
                half = y_ref[K // 2 : K, :].astype(F32)
                size = jnp.sum(half * half, axis=1, keepdims=True)
                a_ref[K // 2 :, K:] = a_ref[K // 2 :, K:] * lax.rsqrt(size)

            @pl.when(step == 2)
            def _():
                for at in range(K // 2, K, PANEL):
                    factor_panel(a_ref, at)

            inverse = a_ref[:, K:]
            inverse = jnp.where(
                lax.broadcasted_iota(jnp.int32, (K, K), 0)
                >= lax.broadcasted_iota(jnp.int32, (K, K), 1),
                inverse, 0.0,
            )
            high = inverse.astype(BF16)
            low = (inverse - high.astype(F32)).astype(BF16)
            for j in range(NB):
                at = slice(j * B, j * B + B)
                x = nn(high, y_ref[:K, at]) + (nn(low, y_ref[:K, at]) + nn(high, y_ref[K:, at]))
                x_ref[:, at] = x
                xb[:, at] = x.astype(BF16)

    core = lax.axis_index("cols")
    own = pl.ds(pl.multiple_of(core * 128, 128), 128)
    basis_ref[...] = x_ref[own, :].T
    wrote = pltpu.make_async_copy(basis_ref, basis_hbm, written.at[steps])
    wrote.start()
    y_ref[:128, :] = xb[own, :]
    y_ref[128:K, :] = xb[pl.ds(pl.multiple_of(128 - core * 128, 128), 128), :]
    parts = [v.astype(F32) for v in split3(jnp.broadcast_to(mean_ref[...], (16, D)))]
    line = lax.broadcasted_iota(jnp.int32, (16, D), 0)
    lines = jnp.where(line == 0, parts[0], jnp.where(line == 1, parts[1], parts[2]))
    lines = jnp.where(line < 3, lines, 0.0).astype(BF16)
    offset[...] = jnp.sum(nt(lines, y_ref[:K, :]), axis=0, keepdims=True)

    def write(step):
        at = pl.ds(pl.multiple_of(step * STEP_ROWS, STEP_ROWS), STEP_ROWS)
        return pltpu.make_async_copy(out_ref.at[at], out_hbm.at[at], written.at[step])

    @pl.loop(0, steps)
    def _(step):
        fetch(step).wait()
        for r in range(0, STEP_ROWS, 256):
            at = pl.ds(pl.multiple_of(step * STEP_ROWS + r, 256), 256)
            coords = (nt(e_ref[at, :], y_ref[:K, :]) - offset[...]) * length_ref[at, :]
            squares = jnp.sum(coords * coords, axis=1, keepdims=True)
            scaled = coords[:, :128] * lax.rsqrt(squares * (1.0 / K) + 0.0001)
            out_ref[at, :] = scaled.astype(BF16)
        write(step).start()

    for step in range(steps):
        write(step).wait()
    wrote.wait()


def finished(embeddings, c_all, apart, mean, b_all, length):
    rows = embeddings.shape[0]
    vm = pl.BlockSpec(memory_space=VMEM)
    hbm = pl.BlockSpec(memory_space=pltpu.HBM)
    return pl.pallas_call(
        finish_kernel,
        out_shape=(
            jax.ShapeDtypeStruct((rows, K // 2), BF16),
            jax.ShapeDtypeStruct((D, K // 2), F32),
        ),
        in_specs=[hbm] + [vm] * 5,
        out_specs=(hbm, hbm),
        scratch_shapes=[
            VMEM((rows, D), BF16),
            VMEM((K, D), F32),
            VMEM((1, K), F32),
            VMEM((K, D), BF16),
            VMEM((K, 2 * K), F32),
            VMEM((2 * K, D), BF16),
            VMEM((rows, K // 2), BF16),
            VMEM((D, K // 2), F32),
            pltpu.SemaphoreType.DMA((rows // STEP_ROWS,)),
            pltpu.SemaphoreType.DMA((rows // STEP_ROWS + 1,)),
        ],
        compiler_params=pltpu.CompilerParams(vmem_limit_bytes=47 * 2**20),
        name="finish",
    )(embeddings, c_all, apart, mean, b_all, length)


def shards(embeddings, start_basis):
    parts = gathered(embeddings, start_basis)
    return tuple(finished(embeddings, *parts))


def solution(mesh):
    in_specs = (P("rows", None), P(None, "cols"))
    out_specs = (P("rows", "cols"), P(None, "cols"))
    return jax.shard_map(shards, mesh=mesh, in_specs=in_specs, out_specs=out_specs, check_vma=False)
```

```python
import functools

import jax
import jax.numpy as jnp
from jax import lax
from jax.experimental import pallas as pl
from jax.experimental.pallas import tpu as pltpu
from jax.sharding import PartitionSpec as P

D = 1536
K = 256
B = 256
NB = D // B
OFFS = 4
MESH = pl.DeviceIdType.MESH
VMEM = pltpu.VMEM
F32 = jnp.float32
BF16 = jnp.bfloat16
STRIDES = (1, 4, 16)
STEP_ROWS = 512
LENGTH_ROWS = 256


def split3(v):
    high = v.astype(BF16)
    rest = v - high.astype(F32)
    mid = rest.astype(BF16)
    low = (rest - mid.astype(F32)).astype(BF16)
    return high, mid, low


def nt(a, b):
    return lax.dot_general(a, b, (((1,), (1,)), ((), ())), preferred_element_type=F32)


def nn(a, b):
    return lax.dot_general(a, b, (((1,), (0,)), ((), ())), preferred_element_type=F32)


def gather_kernel(
    rows, e_hbm, b_ref,
    c_out, apart_out, mean_out, b_out, length_out,
    e_ref, turned, s_ref, mu_ref, mu_out, sums,
    got1, got2, got3, part2, fetched,
    send_rs, recv_rs, send_ag, recv_ag, send_cc, recv_cc, send_mu, recv_mu, send_x, recv_x,
):
    me = lax.axis_index("rows")
    core = lax.axis_index("cols")
    other = 1 - core
    coord = [lax.rem(me // s, 4) for s in STRIDES]
    steps = rows // STEP_ROWS

    def fetch(step):
        at = pl.ds(pl.multiple_of(step * STEP_ROWS, STEP_ROWS), STEP_ROWS)
        return pltpu.make_async_copy(e_hbm.at[at], e_ref.at[at], fetched.at[step])

    for step in range(steps):
        fetch(step).start()

    def peer(dim, o):
        return me + (lax.rem(coord[dim] + o, 4) - coord[dim]) * STRIDES[dim]

    barrier = pltpu.get_barrier_semaphore()
    for dim in range(3):
        for o in (1, 2, 3):
            pl.semaphore_signal(barrier, inc=1, device_id=(peer(dim, o), core), device_id_type=MESH)
    pl.semaphore_signal(barrier, inc=1, device_id=(me, other), device_id_type=MESH)

    sums[...] = jnp.zeros_like(sums)

    @pl.loop(0, steps)
    def _(step):
        fetch(step).wait()
        start = pl.multiple_of(step * STEP_ROWS, STEP_ROWS)
        for k in range(3):
            i = core * 3 + k
            part = e_ref[pl.ds(start, STEP_ROWS), pl.ds(pl.multiple_of(i * B, B), B)]
            turned[k * B : k * B + B, pl.ds(start, STEP_ROWS)] = part.T
        for q in range(NB):
            at = slice(q * B, q * B + B)
            total = sums[:, at]
            for r in range(0, STEP_ROWS, 16):
                total = total + e_ref[pl.ds(start + r, 16), at].astype(F32)
            sums[:, at] = total

    whole = jnp.sum(sums[...], axis=0, keepdims=True)
    mean = whole * (1.0 / rows)
    sums[0:1, :] = mean
    for k in range(3):
        for half in range(2):
            at = pl.ds(pl.multiple_of((core * 3 + k) * B + half * 128, 128), 128)
            mu_ref[2 * k + half : 2 * k + half + 1, :] = sums[0:1, at]
    mu_ref[6:8, :] = jnp.zeros((2, 128), F32)
    place = coord[0] * 16 + coord[1] * 4 + coord[2]
    mu_out[core, place] = mu_ref[...]
    b_out[core] = b_ref[...]

    started = []

    def send(src, dst, send_sem, recv_sem, to):
        copy = pltpu.make_async_remote_copy(
            src_ref=src, dst_ref=dst, send_sem=send_sem, recv_sem=recv_sem,
            device_id=to, device_id_type=MESH,
        )
        copy.start()
        started.append(copy)
        return copy

    def rows_of(k, start, size):
        return pl.ds(pl.multiple_of(k * 1024 + start, 16), size)

    pl.semaphore_wait(barrier, 10)

    def send_means(n, at):
        return [
            send(
                mu_out.at[core, at], mu_out.at[core, at],
                send_mu.at[n, o - 1], recv_mu.at[n, o - 1], (peer(2 - n, o), core),
            )
            for o in (2, 1, 3)
        ]

    means = send_means(0, pl.ds(place, 1))
    b_copy = send(b_ref, b_out.at[core], send_x.at[0], recv_x.at[0], (me, other))

    line = lax.broadcasted_iota(jnp.int32, (16, D), 0)

    def lines(v, order):
        parts = split3(jnp.broadcast_to(v, (16, D)))
        out = jnp.zeros((16, D), F32)
        for n, which in enumerate(order):
            out = jnp.where(line == n, parts[which].astype(F32), out)
        return out.astype(BF16)

    e_ref[rows:, :] = lines(-mean, (0, 1, 0, 1, 2, 0))
    s_ref[:16 * NB, :] = jnp.concatenate(
        [lines(whole, (0, 0, 1, 1, 0, 2))[:, q * B : q * B + B] for q in range(NB)], axis=0
    )
    for k in range(3):
        part = s_ref[pl.ds(pl.multiple_of((core * 3 + k) * 16, 16), 16), :]
        part = jnp.concatenate([part, jnp.zeros((112, B), BF16)], axis=0)
        turned[k * B : k * B + B, rows:] = part.T

    def first_copy(k, o):
        block = rows_of(k, lax.rem(coord[k] + o, 4) * 256, 256)
        return pltpu.make_async_remote_copy(
            src_ref=s_ref.at[block], dst_ref=got1.at[k, o - 1],
            send_sem=send_rs.at[0, k, o - 1], recv_sem=recv_rs.at[0, k, o - 1],
            device_id=(peer(k, o), core), device_id_type=MESH,
        )

    line_of = pl.ds(pl.multiple_of(place // 4 * 4, 4), 4)
    means_next = [
        pltpu.make_async_remote_copy(
            src_ref=mu_out.at[core, line_of], dst_ref=mu_out.at[core, line_of],
            send_sem=send_mu.at[1, o - 1], recv_sem=recv_mu.at[1, o - 1],
            device_id=(peer(1, o), core), device_id_type=MESH,
        )
        for o in (2, 1, 3)
    ]

    @pl.loop(0, 3 * OFFS)
    def _(m):
        n, k = m // 3, lax.rem(m, 3)
        o = 2 + n // 2 - lax.rem(n, 2) * (1 + 2 * (n // 2))
        stride = 1 + k * (9 * k - 3) // 2
        here = lax.rem(me // stride, 4)
        to = lax.rem(here + o, 4)
        at = pl.ds(pl.multiple_of(lax.rem(core * 3 + k + to, NB) * B, B), B)
        left = turned[pl.ds(pl.multiple_of(k * B, B), B), : rows + 16]
        block = rows_of(k, to * 256, 256)
        s_ref[block, :] = nn(left, e_ref[:, at]).astype(BF16)

        @pl.when(o > 0)
        def _():
            pltpu.make_async_remote_copy(
                src_ref=s_ref.at[block], dst_ref=got1.at[k, o - 1],
                send_sem=send_rs.at[0, k, o - 1], recv_sem=recv_rs.at[0, k, o - 1],
                device_id=(me + (to - here) * stride, core), device_id_type=MESH,
            ).start()

        @pl.when(m == 5)
        def _():
            for copy in means:
                copy.wait_recv()
            for copy in means_next:
                copy.start()

    started.extend(means_next)

    second = {}
    for k in range(3):
        for o in (1, 2, 3):
            first_copy(k, o).wait_recv()
        total = s_ref[rows_of(k, coord[k] * 256, 256), :].astype(F32)
        for o in range(3):
            total = total + got1[k, o].astype(F32)
        part2[k] = total.astype(BF16)
        d = (k + 1) % 3
        for o in (2, 1, 3):
            to = lax.rem(coord[d] + o, 4)
            second[k, o] = send(
                part2.at[k, pl.ds(pl.multiple_of(to * 64, 16), 64)], got2.at[k, o - 1],
                send_rs.at[1, k, o - 1], recv_rs.at[1, k, o - 1], (peer(d, o), core),
            )

    for copy in means_next:
        copy.wait_recv()
    means = send_means(2, pl.ds(pl.multiple_of(coord[0] * 16, 16), 16))

    third = {}
    for k in range(3):
        d = (k + 1) % 3
        for o in (1, 2, 3):
            second[k, o].wait_recv()
        total = part2[k, pl.ds(pl.multiple_of(coord[d] * 64, 16), 64), :].astype(F32)
        for o in range(3):
            total = total + got2[k, o].astype(F32)
        d = (k + 2) % 3
        got3[k, coord[d]] = total.astype(BF16)
        for o in (2, 1, 3):
            third[k, o] = send(
                got3.at[k, coord[d]], got3.at[k, coord[d]],
                send_rs.at[2, k, o - 1], recv_rs.at[2, k, o - 1], (peer(d, o), core),
            )
    for copy in means:
        copy.wait_recv()
    mu_copy = send(mu_out.at[core], mu_out.at[core], send_x.at[1], recv_x.at[1], (me, other))
    spread = {}
    for k in range(3):
        a, b = (coord[(k + n) % 3] for n in range(2))
        d = (k + 1) % 3
        for o in (1, 2, 3):
            third[k, o].wait_recv()
        total = got3[k, 0].astype(F32)
        for c in range(1, 4):
            total = total + got3[k, c].astype(F32)
        mine = rows_of(k, (a * 4 + b) * 64, 64)
        c_out[core, mine, :] = total.astype(BF16)
        for o in (2, 1, 3):
            spread[1, k, o] = send(
                c_out.at[core, mine], c_out.at[core, mine],
                send_ag.at[0, k, o - 1], recv_ag.at[0, k, o - 1], (peer(d, o), core),
            )
    across = []
    for k in range(3):
        a = coord[k]
        for o in (1, 2, 3):
            spread[1, k, o].wait_recv()
        mine = rows_of(k, a * 256, 256)
        for o in (2, 1, 3):
            spread[2, k, o] = send(
                c_out.at[core, mine], c_out.at[core, mine],
                send_ag.at[1, k, o - 1], recv_ag.at[1, k, o - 1], (peer(k, o), core),
            )
        across.append(
            send(
                c_out.at[core, mine], c_out.at[core, mine],
                send_cc.at[k, 0], recv_cc.at[k, 0], (me, other),
            )
        )
    mu_copy.wait_recv()
    for h in range(2):
        for q in range(6):
            at = slice((h * 6 + q) * 128, (h * 6 + q + 1) * 128)
            part = mu_out[h, :, q, :]
            center = jnp.mean(part, axis=0, keepdims=True)
            mean_out[:, at] = center
            part = part - center
            high = part.astype(BF16)
            low = (part - high.astype(F32)).astype(BF16)
            apart_out[:, at] = jnp.concatenate([high, low, high, low], axis=0)

    def lengths():
        @pl.loop(0, rows // LENGTH_ROWS)
        def _(n):
            at = pl.ds(pl.multiple_of(n * LENGTH_ROWS, LENGTH_ROWS), LENGTH_ROWS)
            apart = e_ref[at, :].astype(F32) - mean_out[...]
            length_out[at, :] = lax.rsqrt(jnp.sum(apart * apart, axis=1, keepdims=True) + 1.0)

    lengths()

    for o in (1, 3, 2):
        for k in range(3):
            spread[2, k, o].wait_recv()
            got = rows_of(k, lax.rem(coord[k] + 4 - o, 4) * 256, 256)
            across.append(
                send(
                    c_out.at[core, got], c_out.at[core, got],
                    send_cc.at[k, o], recv_cc.at[k, o], (me, other),
                )
            )
    for copy in across:
        copy.wait_recv()
    b_copy.wait_recv()
    for copy in started:
        copy.wait_send()
    for k in range(3):
        for o in (1, 2, 3):
            first_copy(k, o).wait_send()


def gathered(embeddings, b):
    rows = embeddings.shape[0]
    size = 3 * OFFS * B
    sem = pltpu.SemaphoreType.DMA
    vm = pl.BlockSpec(memory_space=VMEM)
    return pl.pallas_call(
        functools.partial(gather_kernel, rows),
        out_shape=(
            jax.ShapeDtypeStruct((2, size, B), BF16),
            jax.ShapeDtypeStruct((K, D), BF16),
            jax.ShapeDtypeStruct((1, D), F32),
            jax.ShapeDtypeStruct((2, K // 2, D), BF16),
            jax.ShapeDtypeStruct((rows, 1), F32),
        ),
        in_specs=[pl.BlockSpec(memory_space=pltpu.HBM), vm],
        out_specs=(vm,) * 5,
        scratch_shapes=[
            VMEM((rows + 16, D), BF16),
            VMEM((3 * B, rows + 128), BF16),
            VMEM((size, B), BF16),
            VMEM((8, 128), F32),
            VMEM((2, 64, 8, 128), F32),
            VMEM((16, D), F32),
            VMEM((3, 3, 256, B), BF16),
            VMEM((3, 3, 64, B), BF16),
            VMEM((3, 4, 64, B), BF16),
            VMEM((3, 256, B), BF16),
            sem((rows // STEP_ROWS,)),
            sem((3, 3, 3)), sem((3, 3, 3)),
            sem((2, 3, 3)), sem((2, 3, 3)),
            sem((3, 4)), sem((3, 4)),
            sem((3, 3)), sem((3, 3)),
            sem((2,)), sem((2,)),
        ],
        compiler_params=pltpu.CompilerParams(
            collective_id=0, has_side_effects=True, vmem_limit_bytes=46 * 2**20
        ),
        name="gather",
    )(embeddings, b)


PANEL = 32
WIDE = 16
ROWS_ALL = 196608.0


def factor_panel(a_ref, at):
    low, high = (0, 3) if at < 128 else (1, 4)
    tiles = range(low, high)
    home = at // 128
    groups = PANEL // 8
    rows = [
        [a_ref[at + 8 * g : at + 8 * g + 8, 128 * t : 128 * t + 128] for t in tiles]
        for g in range(groups)
    ]
    line = lax.broadcasted_iota(jnp.int32, (8, 128), 0)
    def spread(v, sublane):
        return jnp.broadcast_to(v[sublane : sublane + 1, :], (8, 128))

    done = []
    for base in range(0, groups, WIDE // 8):
        first = at + 8 * base - 128 * home
        cols = [
            {
                t: jnp.broadcast_to(
                    rows[t][home - low][:, first + c : first + c + 1], (8, 128)
                )
                for t in range(base + c // 8, groups)
            }
            for c in range(WIDE)
        ]
        pivot = spread(cols[0][base], 0)
        for c in range(WIDE):
            g, j = base + c // 8, c % 8
            root = lax.rsqrt(pivot)
            scale = root if j == 0 else jnp.where(line >= j, root, scale)
            inverse = root * root
            heads = {n: spread(cols[c][base + n // 8], n % 8) for n in range(c + 1, WIDE)}
            if c + 1 < WIDE:
                pivot = spread(cols[c + 1][base + (c + 1) // 8], (c + 1) % 8)
                pivot = pivot - heads[c + 1] * heads[c + 1] * inverse
            source = [spread(v, j) for v in rows[g]]
            for t in range(g, groups):
                m = cols[c][t]
                if t == g:
                    m = jnp.where(line > j, m, 0.0)
                m = m * inverse
                for n in range(c + 1, WIDE):
                    if t >= base + n // 8:
                        cols[n][t] = cols[n][t] - m * heads[n]
                rows[t] = [v - m * s for v, s in zip(rows[t], source)]
            if j == 7:
                rows[g] = [v * scale for v in rows[g]]
                done.append(rows[g])
    for g in range(groups):
        for t, v in zip(tiles, done[g]):
            a_ref[at + 8 * g : at + 8 * g + 8, 128 * t : 128 * t + 128] = v
    left = K - at - PANEL
    if left:
        whole = [jnp.concatenate([done[g][n] for g in range(groups)], axis=0) for n in range(3)]
        whole = jnp.concatenate(whole, axis=1)
        high_, mid, low_ = split3(whole)
        right = jnp.concatenate([high_, mid, high_, low_, high_, mid], axis=0)
        side = jnp.concatenate([high_, high_, mid, high_, low_, mid], axis=0)
        side = side[:, : (2 - low) * 128]
        change = lax.dot_general(
            side, right, (((0,), (0,)), ((), ())), preferred_element_type=F32
        )
        skip = at + PANEL - 128 * low
        cols = slice(128 * low, 128 * high)
        a_ref[at + PANEL : K, cols] = a_ref[at + PANEL : K, cols] - change[skip:, :]


def finish_kernel(
    e_hbm, c_ref, apart, mean_ref, b_ref, length_ref, out_hbm, basis_hbm,
    e_ref, x_ref, offset, xb, a_ref, y_ref, out_ref, basis_ref, fetched, written,
):
    rows = e_ref.shape[0]
    steps = rows // STEP_ROWS

    def fetch(step):
        at = pl.ds(pl.multiple_of(step * STEP_ROWS, STEP_ROWS), STEP_ROWS)
        return pltpu.make_async_copy(e_hbm.at[at], e_ref.at[at], fetched.at[step])

    for step in range(steps):
        fetch(step).start()
    for h in range(2):
        xb[128 * h : 128 * h + 128, :] = b_ref[h]

    @pl.loop(0, 3)
    def _(step):
        t = nt(xb[...], apart[:128, :]) * float(rows)
        t = t + pltpu.roll(t, 64, 1)
        high = t.astype(BF16)
        low = (t - high.astype(F32)).astype(BF16)
        t = jnp.concatenate([high, low], axis=1)
        for j in range(NB):
            at = slice(j * B, j * B + B)
            total = nn(t, apart[:, at])
            for i in range(NB):
                o = (j - i) % NB
                left = xb[:, i * B : i * B + B]
                if o < OFFS:
                    r = (i % 3 * OFFS + o) * B
                    total = total + nn(left, c_ref[i // 3, r : r + B, :])
                else:
                    r = (j % 3 * OFFS + NB - o) * B
                    total = total + nt(left, c_ref[j // 3, r : r + B, :])
            total = total * (1.0 / ROWS_ALL)
            high = total.astype(BF16)
            y_ref[:K, at] = high
            y_ref[K:, at] = (total - high.astype(F32)).astype(BF16)

        @pl.when(step == 0)
        def _():
            xb[...] = y_ref[:K, :]

        @pl.when(step > 0)
        def _():
            def gram(half):
                at = slice(half * 128, half * 128 + 128)
                high = nt(y_ref[at, :], y_ref[...])
                low = nt(y_ref[K + half * 128 : K + half * 128 + 128, :], y_ref[...])
                a_ref[at, :K] = high[:, :K] + low[:, K:] + (high[:, K:] + low[:, :K])

            gram(0)

            @pl.when(step == 1)
            def _():
                a_ref[K // 2 :, :K] = jnp.zeros((K // 2, K), F32)

            @pl.when(step == 2)
            def _():
                gram(1)

            a_ref[:, K:] = (
                lax.broadcasted_iota(jnp.int32, (K, K), 0)
                == lax.broadcasted_iota(jnp.int32, (K, K), 1)
            ).astype(F32)
            for at in range(0, K // 2, PANEL):
                factor_panel(a_ref, at)

            @pl.when(step == 1)
            def _():
                half = y_ref[K // 2 : K, :].astype(F32)
                size = jnp.sum(half * half, axis=1, keepdims=True)
                a_ref[K // 2 :, K:] = a_ref[K // 2 :, K:] * lax.rsqrt(size)

            @pl.when(step == 2)
            def _():
                for at in range(K // 2, K, PANEL):
                    factor_panel(a_ref, at)

            inverse = a_ref[:, K:]
            inverse = jnp.where(
                lax.broadcasted_iota(jnp.int32, (K, K), 0)
                >= lax.broadcasted_iota(jnp.int32, (K, K), 1),
                inverse, 0.0,
            )
            high = inverse.astype(BF16)
            low = (inverse - high.astype(F32)).astype(BF16)
            for j in range(NB):
                at = slice(j * B, j * B + B)
                x = nn(high, y_ref[:K, at]) + (nn(low, y_ref[:K, at]) + nn(high, y_ref[K:, at]))
                x_ref[:, at] = x
                xb[:, at] = x.astype(BF16)

    core = lax.axis_index("cols")
    own = pl.ds(pl.multiple_of(core * 128, 128), 128)
    basis_ref[...] = x_ref[own, :].T
    wrote = pltpu.make_async_copy(basis_ref, basis_hbm, written.at[steps])
    wrote.start()
    y_ref[:128, :] = xb[own, :]
    y_ref[128:K, :] = xb[pl.ds(pl.multiple_of(128 - core * 128, 128), 128), :]
    parts = [v.astype(F32) for v in split3(jnp.broadcast_to(mean_ref[...], (16, D)))]
    line = lax.broadcasted_iota(jnp.int32, (16, D), 0)
    lines = jnp.where(line == 0, parts[0], jnp.where(line == 1, parts[1], parts[2]))
    lines = jnp.where(line < 3, lines, 0.0).astype(BF16)
    offset[...] = jnp.sum(nt(lines, y_ref[:K, :]), axis=0, keepdims=True)

    def write(step):
        at = pl.ds(pl.multiple_of(step * STEP_ROWS, STEP_ROWS), STEP_ROWS)
        return pltpu.make_async_copy(out_ref.at[at], out_hbm.at[at], written.at[step])

    @pl.loop(0, steps)
    def _(step):
        fetch(step).wait()
        for r in range(0, STEP_ROWS, 256):
            at = pl.ds(pl.multiple_of(step * STEP_ROWS + r, 256), 256)
            coords = (nt(e_ref[at, :], y_ref[:K, :]) - offset[...]) * length_ref[at, :]
            squares = jnp.sum(coords * coords, axis=1, keepdims=True)
            scaled = coords[:, :128] * lax.rsqrt(squares * (1.0 / K) + 0.0001)
            out_ref[at, :] = scaled.astype(BF16)
        write(step).start()

    for step in range(steps):
        write(step).wait()
    wrote.wait()


def finished(embeddings, c_all, apart, mean, b_all, length):
    rows = embeddings.shape[0]
    vm = pl.BlockSpec(memory_space=VMEM)
    hbm = pl.BlockSpec(memory_space=pltpu.HBM)
    return pl.pallas_call(
        finish_kernel,
        out_shape=(
            jax.ShapeDtypeStruct((rows, K // 2), BF16),
            jax.ShapeDtypeStruct((D, K // 2), F32),
        ),
        in_specs=[hbm] + [vm] * 5,
        out_specs=(hbm, hbm),
        scratch_shapes=[
            VMEM((rows, D), BF16),
            VMEM((K, D), F32),
            VMEM((1, K), F32),
            VMEM((K, D), BF16),
            VMEM((K, 2 * K), F32),
            VMEM((2 * K, D), BF16),
            VMEM((rows, K // 2), BF16),
            VMEM((D, K // 2), F32),
            pltpu.SemaphoreType.DMA((rows // STEP_ROWS,)),
            pltpu.SemaphoreType.DMA((rows // STEP_ROWS + 1,)),
        ],
        compiler_params=pltpu.CompilerParams(vmem_limit_bytes=47 * 2**20),
        name="finish",
    )(embeddings, c_all, apart, mean, b_all, length)


def shards(embeddings, start_basis):
    parts = gathered(embeddings, start_basis.T.astype(BF16))
    return tuple(finished(embeddings, *parts))


def solution(mesh):
    in_specs = (P("rows", None), P(None, "cols"))
    out_specs = (P("rows", "cols"), P(None, "cols"))
    return jax.shard_map(shards, mesh=mesh, in_specs=in_specs, out_specs=out_specs, check_vma=False)
```

```python
import functools

import jax
import jax.numpy as jnp
from jax import lax
from jax.experimental import pallas as pl
from jax.experimental.pallas import tpu as pltpu
from jax.sharding import PartitionSpec as P

D = 1536
K = 256
B = 256
NB = D // B
OFFS = 4
MESH = pl.DeviceIdType.MESH
VMEM = pltpu.VMEM
F32 = jnp.float32
BF16 = jnp.bfloat16
STRIDES = (1, 4, 16)
STEP_ROWS = 512
LENGTH_ROWS = 256


def split3(v):
    high = v.astype(BF16)
    rest = v - high.astype(F32)
    mid = rest.astype(BF16)
    low = (rest - mid.astype(F32)).astype(BF16)
    return high, mid, low


def nt(a, b):
    return lax.dot_general(a, b, (((1,), (1,)), ((), ())), preferred_element_type=F32)


def nn(a, b):
    return lax.dot_general(a, b, (((1,), (0,)), ((), ())), preferred_element_type=F32)


def gather_kernel(
    rows, e_hbm, b_ref,
    c_out, apart_out, mean_out, b_out, length_out,
    e_ref, turned, s_ref, mu_ref, mu_out, sums,
    got1, got2, got3, part2, fetched,
    send_rs, recv_rs, send_ag, recv_ag, send_cc, recv_cc, send_mu, recv_mu, send_x, recv_x,
):
    me = lax.axis_index("rows")
    core = lax.axis_index("cols")
    other = 1 - core
    coord = [lax.rem(me // s, 4) for s in STRIDES]
    steps = rows // STEP_ROWS

    def fetch(step):
        at = pl.ds(pl.multiple_of(step * STEP_ROWS, STEP_ROWS), STEP_ROWS)
        return pltpu.make_async_copy(e_hbm.at[at], e_ref.at[at], fetched.at[step])

    for step in range(steps):
        fetch(step).start()

    def peer(dim, o):
        return me + (lax.rem(coord[dim] + o, 4) - coord[dim]) * STRIDES[dim]

    barrier = pltpu.get_barrier_semaphore()
    for dim in range(3):
        for o in (1, 2, 3):
            pl.semaphore_signal(barrier, inc=1, device_id=(peer(dim, o), core), device_id_type=MESH)
    pl.semaphore_signal(barrier, inc=1, device_id=(me, other), device_id_type=MESH)

    sums[...] = jnp.zeros_like(sums)

    @pl.loop(0, steps)
    def _(step):
        fetch(step).wait()
        start = pl.multiple_of(step * STEP_ROWS, STEP_ROWS)
        for k in range(3):
            i = core * 3 + k
            part = e_ref[pl.ds(start, STEP_ROWS), pl.ds(pl.multiple_of(i * B, B), B)]
            turned[k * B : k * B + B, pl.ds(start, STEP_ROWS)] = part.T
        for q in range(NB):
            at = slice(q * B, q * B + B)
            total = sums[:, at]
            for r in range(0, STEP_ROWS, 16):
                total = total + e_ref[pl.ds(start + r, 16), at].astype(F32)
            sums[:, at] = total

    whole = jnp.sum(sums[...], axis=0, keepdims=True)
    mean = whole * (1.0 / rows)
    sums[0:1, :] = mean
    for k in range(3):
        for half in range(2):
            at = pl.ds(pl.multiple_of((core * 3 + k) * B + half * 128, 128), 128)
            mu_ref[2 * k + half : 2 * k + half + 1, :] = sums[0:1, at]
    mu_ref[6:8, :] = jnp.zeros((2, 128), F32)
    place = coord[0] * 16 + coord[1] * 4 + coord[2]
    mu_out[core, place] = mu_ref[...]
    b_out[core] = b_ref[...]

    started = []

    def send(src, dst, send_sem, recv_sem, to):
        copy = pltpu.make_async_remote_copy(
            src_ref=src, dst_ref=dst, send_sem=send_sem, recv_sem=recv_sem,
            device_id=to, device_id_type=MESH,
        )
        copy.start()
        started.append(copy)
        return copy

    def rows_of(k, start, size):
        return pl.ds(pl.multiple_of(k * 1024 + start, 16), size)

    pl.semaphore_wait(barrier, 10)

    def send_means(n, at):
        return [
            send(
                mu_out.at[core, at], mu_out.at[core, at],
                send_mu.at[n, o - 1], recv_mu.at[n, o - 1], (peer(2 - n, o), core),
            )
            for o in (2, 1, 3)
        ]

    means = send_means(0, pl.ds(place, 1))
    b_copy = send(b_ref, b_out.at[core], send_x.at[0], recv_x.at[0], (me, other))

    line = lax.broadcasted_iota(jnp.int32, (16, D), 0)

    def lines(v, order):
        parts = split3(jnp.broadcast_to(v, (16, D)))
        out = jnp.zeros((16, D), F32)
        for n, which in enumerate(order):
            out = jnp.where(line == n, parts[which].astype(F32), out)
        return out.astype(BF16)

    e_ref[rows:, :] = lines(-mean, (0, 1, 0, 1, 2, 0))
    s_ref[:16 * NB, :] = jnp.concatenate(
        [lines(whole, (0, 0, 1, 1, 0, 2))[:, q * B : q * B + B] for q in range(NB)], axis=0
    )
    for k in range(3):
        part = s_ref[pl.ds(pl.multiple_of((core * 3 + k) * 16, 16), 16), :]
        part = jnp.concatenate([part, jnp.zeros((112, B), BF16)], axis=0)
        turned[k * B : k * B + B, rows:] = part.T

    def first_copy(k, o):
        block = rows_of(k, lax.rem(coord[k] + o, 4) * 256, 256)
        return pltpu.make_async_remote_copy(
            src_ref=s_ref.at[block], dst_ref=got1.at[k, o - 1],
            send_sem=send_rs.at[0, k, o - 1], recv_sem=recv_rs.at[0, k, o - 1],
            device_id=(peer(k, o), core), device_id_type=MESH,
        )

    line_of = pl.ds(pl.multiple_of(place // 4 * 4, 4), 4)
    means_next = [
        pltpu.make_async_remote_copy(
            src_ref=mu_out.at[core, line_of], dst_ref=mu_out.at[core, line_of],
            send_sem=send_mu.at[1, o - 1], recv_sem=recv_mu.at[1, o - 1],
            device_id=(peer(1, o), core), device_id_type=MESH,
        )
        for o in (2, 1, 3)
    ]

    @pl.loop(0, 3 * OFFS)
    def _(m):
        n, k = m // 3, lax.rem(m, 3)
        o = 2 + n // 2 - lax.rem(n, 2) * (1 + 2 * (n // 2))
        stride = 1 + k * (9 * k - 3) // 2
        here = lax.rem(me // stride, 4)
        to = lax.rem(here + o, 4)
        at = pl.ds(pl.multiple_of(lax.rem(core * 3 + k + to, NB) * B, B), B)
        left = turned[pl.ds(pl.multiple_of(k * B, B), B), : rows + 16]
        block = rows_of(k, to * 256, 256)
        s_ref[block, :] = nn(left, e_ref[:, at]).astype(BF16)

        @pl.when(o > 0)
        def _():
            pltpu.make_async_remote_copy(
                src_ref=s_ref.at[block], dst_ref=got1.at[k, o - 1],
                send_sem=send_rs.at[0, k, o - 1], recv_sem=recv_rs.at[0, k, o - 1],
                device_id=(me + (to - here) * stride, core), device_id_type=MESH,
            ).start()

        @pl.when(m == 5)
        def _():
            for copy in means:
                copy.wait_recv()
            for copy in means_next:
                copy.start()

    started.extend(means_next)

    second = {}
    for k in range(3):
        for o in (1, 2, 3):
            first_copy(k, o).wait_recv()
        total = s_ref[rows_of(k, coord[k] * 256, 256), :].astype(F32)
        for o in range(3):
            total = total + got1[k, o].astype(F32)
        part2[k] = total.astype(BF16)
        d = (k + 1) % 3
        for o in (2, 1, 3):
            to = lax.rem(coord[d] + o, 4)
            second[k, o] = send(
                part2.at[k, pl.ds(pl.multiple_of(to * 64, 16), 64)], got2.at[k, o - 1],
                send_rs.at[1, k, o - 1], recv_rs.at[1, k, o - 1], (peer(d, o), core),
            )

    for copy in means_next:
        copy.wait_recv()
    means = send_means(2, pl.ds(pl.multiple_of(coord[0] * 16, 16), 16))

    third = {}
    for k in range(3):
        d = (k + 1) % 3
        for o in (1, 2, 3):
            second[k, o].wait_recv()
        total = part2[k, pl.ds(pl.multiple_of(coord[d] * 64, 16), 64), :].astype(F32)
        for o in range(3):
            total = total + got2[k, o].astype(F32)
        d = (k + 2) % 3
        got3[k, coord[d]] = total.astype(BF16)
        for o in (2, 1, 3):
            third[k, o] = send(
                got3.at[k, coord[d]], got3.at[k, coord[d]],
                send_rs.at[2, k, o - 1], recv_rs.at[2, k, o - 1], (peer(d, o), core),
            )
    for copy in means:
        copy.wait_recv()
    mu_copy = send(mu_out.at[core], mu_out.at[core], send_x.at[1], recv_x.at[1], (me, other))
    spread = {}
    for k in range(3):
        a, b = (coord[(k + n) % 3] for n in range(2))
        d = (k + 1) % 3
        for o in (1, 2, 3):
            third[k, o].wait_recv()
        total = got3[k, 0].astype(F32)
        for c in range(1, 4):
            total = total + got3[k, c].astype(F32)
        mine = rows_of(k, (a * 4 + b) * 64, 64)
        c_out[core, mine, :] = total.astype(BF16)
        for o in (2, 1, 3):
            spread[1, k, o] = send(
                c_out.at[core, mine], c_out.at[core, mine],
                send_ag.at[0, k, o - 1], recv_ag.at[0, k, o - 1], (peer(d, o), core),
            )
    mu_copy.wait_recv()
    for h in range(2):
        for q in range(6):
            at = slice((h * 6 + q) * 128, (h * 6 + q + 1) * 128)
            part = mu_out[h, :, q, :]
            center = jnp.mean(part, axis=0, keepdims=True)
            mean_out[:, at] = center
            part = part - center
            high = part.astype(BF16)
            low = (part - high.astype(F32)).astype(BF16)
            apart_out[:, at] = jnp.concatenate([high, low, high, low], axis=0)

    def lengths(part):
        half = rows // LENGTH_ROWS // 2

        @pl.loop(part * half, part * half + half)
        def _(n):
            at = pl.ds(pl.multiple_of(n * LENGTH_ROWS, LENGTH_ROWS), LENGTH_ROWS)
            apart = e_ref[at, :].astype(F32) - mean_out[...]
            length_out[at, :] = lax.rsqrt(jnp.sum(apart * apart, axis=1, keepdims=True) + 1.0)

    lengths(0)

    across = []
    for k in range(3):
        a = coord[k]
        for o in (1, 2, 3):
            spread[1, k, o].wait_recv()
        mine = rows_of(k, a * 256, 256)
        for o in (2, 1, 3):
            spread[2, k, o] = send(
                c_out.at[core, mine], c_out.at[core, mine],
                send_ag.at[1, k, o - 1], recv_ag.at[1, k, o - 1], (peer(k, o), core),
            )
        across.append(
            send(
                c_out.at[core, mine], c_out.at[core, mine],
                send_cc.at[k, 0], recv_cc.at[k, 0], (me, other),
            )
        )
    lengths(1)
    for o in (1, 3, 2):
        for k in range(3):
            spread[2, k, o].wait_recv()
            got = rows_of(k, lax.rem(coord[k] + 4 - o, 4) * 256, 256)
            across.append(
                send(
                    c_out.at[core, got], c_out.at[core, got],
                    send_cc.at[k, o], recv_cc.at[k, o], (me, other),
                )
            )
    for copy in across:
        copy.wait_recv()
    b_copy.wait_recv()
    for copy in started:
        copy.wait_send()
    for k in range(3):
        for o in (1, 2, 3):
            first_copy(k, o).wait_send()


def gathered(embeddings, b):
    rows = embeddings.shape[0]
    size = 3 * OFFS * B
    sem = pltpu.SemaphoreType.DMA
    vm = pl.BlockSpec(memory_space=VMEM)
    return pl.pallas_call(
        functools.partial(gather_kernel, rows),
        out_shape=(
            jax.ShapeDtypeStruct((2, size, B), BF16),
            jax.ShapeDtypeStruct((K, D), BF16),
            jax.ShapeDtypeStruct((1, D), F32),
            jax.ShapeDtypeStruct((2, K // 2, D), BF16),
            jax.ShapeDtypeStruct((rows, 1), F32),
        ),
        in_specs=[pl.BlockSpec(memory_space=pltpu.HBM), vm],
        out_specs=(vm,) * 5,
        scratch_shapes=[
            VMEM((rows + 16, D), BF16),
            VMEM((3 * B, rows + 128), BF16),
            VMEM((size, B), BF16),
            VMEM((8, 128), F32),
            VMEM((2, 64, 8, 128), F32),
            VMEM((16, D), F32),
            VMEM((3, 3, 256, B), BF16),
            VMEM((3, 3, 64, B), BF16),
            VMEM((3, 4, 64, B), BF16),
            VMEM((3, 256, B), BF16),
            sem((rows // STEP_ROWS,)),
            sem((3, 3, 3)), sem((3, 3, 3)),
            sem((2, 3, 3)), sem((2, 3, 3)),
            sem((3, 4)), sem((3, 4)),
            sem((3, 3)), sem((3, 3)),
            sem((2,)), sem((2,)),
        ],
        compiler_params=pltpu.CompilerParams(
            collective_id=0, has_side_effects=True, vmem_limit_bytes=46 * 2**20
        ),
        name="gather",
    )(embeddings, b)


PANEL = 32
WIDE = 16
ROWS_ALL = 196608.0


def factor_panel(a_ref, at):
    low, high = (0, 3) if at < 128 else (1, 4)
    tiles = range(low, high)
    home = at // 128
    groups = PANEL // 8
    rows = [
        [a_ref[at + 8 * g : at + 8 * g + 8, 128 * t : 128 * t + 128] for t in tiles]
        for g in range(groups)
    ]
    line = lax.broadcasted_iota(jnp.int32, (8, 128), 0)
    def spread(v, sublane):
        return jnp.broadcast_to(v[sublane : sublane + 1, :], (8, 128))

    done = []
    for base in range(0, groups, WIDE // 8):
        first = at + 8 * base - 128 * home
        cols = [
            {
                t: jnp.broadcast_to(
                    rows[t][home - low][:, first + c : first + c + 1], (8, 128)
                )
                for t in range(base + c // 8, groups)
            }
            for c in range(WIDE)
        ]
        pivot = spread(cols[0][base], 0)
        for c in range(WIDE):
            g, j = base + c // 8, c % 8
            root = lax.rsqrt(pivot)
            scale = root if j == 0 else jnp.where(line >= j, root, scale)
            inverse = root * root
            heads = {n: spread(cols[c][base + n // 8], n % 8) for n in range(c + 1, WIDE)}
            if c + 1 < WIDE:
                pivot = spread(cols[c + 1][base + (c + 1) // 8], (c + 1) % 8)
                pivot = pivot - heads[c + 1] * heads[c + 1] * inverse
            source = [spread(v, j) for v in rows[g]]
            for t in range(g, groups):
                m = cols[c][t]
                if t == g:
                    m = jnp.where(line > j, m, 0.0)
                m = m * inverse
                for n in range(c + 1, WIDE):
                    if t >= base + n // 8:
                        cols[n][t] = cols[n][t] - m * heads[n]
                rows[t] = [v - m * s for v, s in zip(rows[t], source)]
            if j == 7:
                rows[g] = [v * scale for v in rows[g]]
                done.append(rows[g])
    for g in range(groups):
        for t, v in zip(tiles, done[g]):
            a_ref[at + 8 * g : at + 8 * g + 8, 128 * t : 128 * t + 128] = v
    left = K - at - PANEL
    if left:
        whole = [jnp.concatenate([done[g][n] for g in range(groups)], axis=0) for n in range(3)]
        whole = jnp.concatenate(whole, axis=1)
        high_, mid, low_ = split3(whole)
        right = jnp.concatenate([high_, mid, high_, low_, high_, mid], axis=0)
        side = jnp.concatenate([high_, high_, mid, high_, low_, mid], axis=0)
        side = side[:, : (2 - low) * 128]
        change = lax.dot_general(
            side, right, (((0,), (0,)), ((), ())), preferred_element_type=F32
        )
        skip = at + PANEL - 128 * low
        cols = slice(128 * low, 128 * high)
        a_ref[at + PANEL : K, cols] = a_ref[at + PANEL : K, cols] - change[skip:, :]


def finish_kernel(
    e_hbm, c_ref, apart, mean_ref, b_ref, length_ref, out_hbm, basis_hbm,
    e_ref, x_ref, offset, xb, a_ref, y_ref, out_ref, basis_ref, fetched, written,
):
    rows = e_ref.shape[0]
    steps = rows // STEP_ROWS

    def fetch(step):
        at = pl.ds(pl.multiple_of(step * STEP_ROWS, STEP_ROWS), STEP_ROWS)
        return pltpu.make_async_copy(e_hbm.at[at], e_ref.at[at], fetched.at[step])

    for step in range(steps):
        fetch(step).start()
    for h in range(2):
        xb[128 * h : 128 * h + 128, :] = b_ref[h]

    @pl.loop(0, 3)
    def _(step):
        t = nt(xb[...], apart[:128, :]) * float(rows)
        t = t + pltpu.roll(t, 64, 1)
        high = t.astype(BF16)
        low = (t - high.astype(F32)).astype(BF16)
        t = jnp.concatenate([high, low], axis=1)
        for j in range(NB):
            at = slice(j * B, j * B + B)
            total = nn(t, apart[:, at])
            for i in range(NB):
                o = (j - i) % NB
                left = xb[:, i * B : i * B + B]
                if o < OFFS:
                    r = (i % 3 * OFFS + o) * B
                    total = total + nn(left, c_ref[i // 3, r : r + B, :])
                else:
                    r = (j % 3 * OFFS + NB - o) * B
                    total = total + nt(left, c_ref[j // 3, r : r + B, :])
            total = total * (1.0 / ROWS_ALL)
            high = total.astype(BF16)
            y_ref[:K, at] = high
            y_ref[K:, at] = (total - high.astype(F32)).astype(BF16)

        @pl.when(step == 0)
        def _():
            xb[...] = y_ref[:K, :]

        @pl.when(step > 0)
        def _():
            def gram(half):
                at = slice(half * 128, half * 128 + 128)
                high = nt(y_ref[at, :], y_ref[...])
                low = nt(y_ref[K + half * 128 : K + half * 128 + 128, :], y_ref[...])
                a_ref[at, :K] = high[:, :K] + low[:, K:] + (high[:, K:] + low[:, :K])

            gram(0)

            @pl.when(step == 1)
            def _():
                a_ref[K // 2 :, :K] = jnp.zeros((K // 2, K), F32)

            @pl.when(step == 2)
            def _():
                gram(1)

            a_ref[:, K:] = (
                lax.broadcasted_iota(jnp.int32, (K, K), 0)
                == lax.broadcasted_iota(jnp.int32, (K, K), 1)
            ).astype(F32)
            for at in range(0, K // 2, PANEL):
                factor_panel(a_ref, at)

            @pl.when(step == 1)
            def _():
                half = y_ref[K // 2 : K, :].astype(F32)
                size = jnp.sum(half * half, axis=1, keepdims=True)
                a_ref[K // 2 :, K:] = a_ref[K // 2 :, K:] * lax.rsqrt(size)

            @pl.when(step == 2)
            def _():
                for at in range(K // 2, K, PANEL):
                    factor_panel(a_ref, at)

            inverse = a_ref[:, K:]
            inverse = jnp.where(
                lax.broadcasted_iota(jnp.int32, (K, K), 0)
                >= lax.broadcasted_iota(jnp.int32, (K, K), 1),
                inverse, 0.0,
            )
            high = inverse.astype(BF16)
            low = (inverse - high.astype(F32)).astype(BF16)
            for j in range(NB):
                at = slice(j * B, j * B + B)
                x = nn(high, y_ref[:K, at]) + (nn(low, y_ref[:K, at]) + nn(high, y_ref[K:, at]))
                x_ref[:, at] = x
                xb[:, at] = x.astype(BF16)

    core = lax.axis_index("cols")
    own = pl.ds(pl.multiple_of(core * 128, 128), 128)
    basis_ref[...] = x_ref[own, :].T
    wrote = pltpu.make_async_copy(basis_ref, basis_hbm, written.at[steps])
    wrote.start()
    y_ref[:128, :] = xb[own, :]
    y_ref[128:K, :] = xb[pl.ds(pl.multiple_of(128 - core * 128, 128), 128), :]
    parts = [v.astype(F32) for v in split3(jnp.broadcast_to(mean_ref[...], (16, D)))]
    line = lax.broadcasted_iota(jnp.int32, (16, D), 0)
    lines = jnp.where(line == 0, parts[0], jnp.where(line == 1, parts[1], parts[2]))
    lines = jnp.where(line < 3, lines, 0.0).astype(BF16)
    offset[...] = jnp.sum(nt(lines, y_ref[:K, :]), axis=0, keepdims=True)

    def write(step):
        at = pl.ds(pl.multiple_of(step * STEP_ROWS, STEP_ROWS), STEP_ROWS)
        return pltpu.make_async_copy(out_ref.at[at], out_hbm.at[at], written.at[step])

    @pl.loop(0, steps)
    def _(step):
        fetch(step).wait()
        for r in range(0, STEP_ROWS, 256):
            at = pl.ds(pl.multiple_of(step * STEP_ROWS + r, 256), 256)
            coords = (nt(e_ref[at, :], y_ref[:K, :]) - offset[...]) * length_ref[at, :]
            squares = jnp.sum(coords * coords, axis=1, keepdims=True)
            scaled = coords[:, :128] * lax.rsqrt(squares * (1.0 / K) + 0.0001)
            out_ref[at, :] = scaled.astype(BF16)
        write(step).start()

    for step in range(steps):
        write(step).wait()
    wrote.wait()


def finished(embeddings, c_all, apart, mean, b_all, length):
    rows = embeddings.shape[0]
    vm = pl.BlockSpec(memory_space=VMEM)
    hbm = pl.BlockSpec(memory_space=pltpu.HBM)
    return pl.pallas_call(
        finish_kernel,
        out_shape=(
            jax.ShapeDtypeStruct((rows, K // 2), BF16),
            jax.ShapeDtypeStruct((D, K // 2), F32),
        ),
        in_specs=[hbm] + [vm] * 5,
        out_specs=(hbm, hbm),
        scratch_shapes=[
            VMEM((rows, D), BF16),
            VMEM((K, D), F32),
            VMEM((1, K), F32),
            VMEM((K, D), BF16),
            VMEM((K, 2 * K), F32),
            VMEM((2 * K, D), BF16),
            VMEM((rows, K // 2), BF16),
            VMEM((D, K // 2), F32),
            pltpu.SemaphoreType.DMA((rows // STEP_ROWS,)),
            pltpu.SemaphoreType.DMA((rows // STEP_ROWS + 1,)),
        ],
        compiler_params=pltpu.CompilerParams(vmem_limit_bytes=47 * 2**20),
        name="finish",
    )(embeddings, c_all, apart, mean, b_all, length)


def shards(embeddings, start_basis):
    parts = gathered(embeddings, start_basis.T.astype(BF16))
    return tuple(finished(embeddings, *parts))


def solution(mesh):
    in_specs = (P("rows", None), P(None, "cols"))
    out_specs = (P("rows", "cols"), P(None, "cols"))
    return jax.shard_map(shards, mesh=mesh, in_specs=in_specs, out_specs=out_specs, check_vma=False)
```
